128 devices in a mesh: tm: 8 (over x_lo, y), space: 16 (over z, x_hi, core).
Axes of the slice: x: 4 (x_hi: 2, x_lo: 2; x = x_hi * 2 + x_lo), y: 4, z: 4, core: 2. Of those that a mesh axis runs over, the one named last changes fastest.
Arguments:
- thermal_field: float32 [512, 196608], P(('tm', 'space')), may hold values from 245 to 255
- seasonal_bucket: int32 [512], replicated, may hold values from 0 to 45, as said below
- season_of_record: int32 [512], replicated, may hold values from 0 to 7
Outputs:
- anomaly: float32 [512, 196608], P(('tm', 'space'))
The draws below stay inside these ranges and needn't reach their ends.
Inputs may be any that keep to these rules, and one draw needn't show every extreme that they name: `seasonal_bucket`: every group holds at least one day whose year is below 6.
All inputs are finite; a program needn't handle non-finite values.
Results may differ from the reference program's by a relative error of at most 0.0003.
Values sent between devices are 32-bit elements; how exact they have to be, the bound alone decides.
A program may use at most 64 MiB of HBM per device.

```python
import jax
import jax.numpy as jnp
from jax import lax

GROUPS = 46
YEARS = 8
BASE_YEARS = 6
TIME_STEPS = 512
MESH_POINTS = 196608


def calendar(key):
    ordering = jax.random.permutation(jax.random.fold_in(key, 11), TIME_STEPS)
    chosen_records = ordering[:GROUPS]
    random_group = jax.random.randint(jax.random.fold_in(key, 12), (TIME_STEPS,), 0, GROUPS)
    random_year = jax.random.randint(jax.random.fold_in(key, 13), (TIME_STEPS,), 0, YEARS)
    base_year = jax.random.randint(jax.random.fold_in(key, 14), (GROUPS,), 0, BASE_YEARS)
    groups = random_group.at[chosen_records].set(jnp.arange(GROUPS, dtype=jnp.int32))
    years = random_year.at[chosen_records].set(base_year)
    return (groups.astype(jnp.int32), years.astype(jnp.int32))


def draw_seasonal_bucket(key, part):
    return calendar(key)[0]


def draw_season_of_record(key, part):
    return calendar(key)[1]


def steps_of(rng, shape, pieces, least, high):
    def one(dim, blocks):
        steps = jax.random.uniform(jax.random.fold_in(jax.random.fold_in(rng, 6), dim), (blocks,), jnp.float32, least / len(pieces), high / len(pieces))
        return jnp.repeat(jnp.exp(steps), shape[dim] // blocks).reshape((-1,) + (1,) * (len(shape) - dim - 1))

    level = one(*pieces[0])
    for cut in pieces[1:]:
        level = level * one(*cut)
    return level


def setup_inputs(seed: int = 0) -> dict:
    splits = jax.random.split(jax.random.key(seed), 4)
    return {
        "thermal_field": jnp.clip(245.0 + 10.0 * jax.random.uniform(splits[0], (TIME_STEPS, MESH_POINTS), jnp.float32) ** steps_of(splits[0], (TIME_STEPS, MESH_POINTS), ((0, 128),), -0.2, 0.2), 245.0, 255.0),
        "seasonal_bucket": draw_seasonal_bucket(jax.random.fold_in(splits[3], 71), 0),
        "season_of_record": draw_season_of_record(jax.random.fold_in(splits[3], 71), 0),
    }


def reference(thermal_field, seasonal_bucket, season_of_record):
    group_ids = jnp.arange(GROUPS, dtype=jnp.int32)
    member = (seasonal_bucket[None, :] == group_ids[:, None]).astype(jnp.float32)
    reference_seasons = member * (season_of_record < BASE_YEARS).astype(jnp.float32)[None, :]
    counts = jnp.sum(reference_seasons, axis=1)
    bucket_aggregates = jnp.dot(reference_seasons, thermal_field, precision=lax.Precision.HIGHEST, preferred_element_type=jnp.float32)
    climate = bucket_aggregates / counts[:, None]
    chosen_records = jnp.dot(member.T, climate, precision=lax.Precision.HIGHEST, preferred_element_type=jnp.float32)
    return thermal_field - chosen_records
```

```python
import functools

import jax
import jax.numpy as jnp
from jax import lax
from jax.experimental import pallas as pl
from jax.experimental.pallas import tpu as pltpu
from jax.sharding import PartitionSpec as P

GROUPS = 46
BASE_YEARS = 6
MESH = pl.DeviceIdType.MESH
F32, BF16 = jnp.float32, jnp.bfloat16

Q = 4
HALF = 48
ROWS = 2 * HALF
PART = ROWS // 4


def coordinates():
    tm, space = lax.axis_index("tm"), lax.axis_index("space")
    x = lax.rem(lax.div(space, 2), 2) * 2 + lax.div(tm, 4)
    return (x, lax.rem(tm, 4), lax.div(space, 4), lax.rem(space, 2))


def device(x, y, z, core):
    return (lax.rem(x, 2) * 4 + y, z * 4 + lax.div(x, 2) * 2 + core)


def peer(me, axis, step, core_step=0):
    at = list(me)
    at[axis] = lax.rem(me[axis] + step, 4)
    at[3] = lax.rem(me[3] + core_step, 2)
    return at


def split(v):
    high = v.astype(BF16)
    rest = v - high.astype(F32)
    middle = rest.astype(BF16)
    low = (rest - middle.astype(F32)).astype(BF16)
    return high, middle, low


def dot3(one_hot, v):
    high, middle, low = split(v)
    dot = functools.partial(jnp.dot, preferred_element_type=F32)
    return dot(one_hot, high) + (dot(one_hot, middle) + dot(one_hot, low))


def kernel(
    x_ref, bucket_row, year_row, bucket_hbm, year_hbm, out_ref,
    buf_a, buf_b, part, got, climate, buf_y, buf_z, member, base_t, counts,
    bucket, year, recv, sent, small,
):
    me = coordinates()
    tiles = x_ref.shape[0] // 3
    chunk = tiles // Q
    na, nb = chunk // 8, chunk // 32

    load_bucket = pltpu.make_async_copy(bucket_hbm, bucket, small.at[0])
    load_year = pltpu.make_async_copy(year_hbm, year, small.at[1])
    load_bucket.start()
    load_year.start()

    barrier = pltpu.get_barrier_semaphore()
    partners = 0
    for axis in range(3):
        for step in range(1, 4):
            for core in range(2):
                pl.semaphore_signal(barrier, inc=1, device_id=device(*peer(me, axis, step, core)), device_id_type=MESH)
                partners += 1
    pl.semaphore_signal(barrier, inc=1, device_id=device(*peer(me, 0, 0, 1)), device_id_type=MESH)
    pl.semaphore_wait(barrier, partners + 1)

    def remote(src, dst, stage, t, q, to):
        pltpu.make_async_remote_copy(
            src_ref=src, dst_ref=dst, send_sem=sent.at[stage], recv_sem=recv.at[stage, t, q],
            device_id=device(*to), device_id_type=MESH,
        ).start()

    def local(src, dst, stage, t, q):
        pltpu.make_async_copy(src, dst, recv.at[stage, t, q]).start()

    def arrive(ref, stage, t, q):
        pltpu.make_async_copy(ref, ref, recv.at[stage, t, q]).wait()

    def axes(t):
        return t, (t + 1) % 3, (t + 2) % 3

    order = ((1, 0), (3, 0), (2, 0), (1, 1), (3, 1), (2, 1), (0, 1))

    def send_a(q):
        for t in range(3):
            mine = me[t] * 2 + me[3]
            local(x_ref.at[pl.ds(t * tiles + q * chunk + mine * na, na)], buf_a.at[t, q, mine], 0, t, q)
        for step, core in order:
            for t in range(3):
                to = peer(me, t, step, core)
                mine, theirs = me[t] * 2 + me[3], to[t] * 2 + to[3]
                remote(x_ref.at[pl.ds(t * tiles + q * chunk + theirs * na, na)], buf_a.at[t, q, mine], 0, t, q, to)

    def send_b(q):
        for t in range(3):
            _, b, _ = axes(t)
            arrive(buf_a.at[t, q], 0, t, q)
            for step in (1, 3, 2):
                to = peer(me, b, step)
                remote(buf_a.at[t, q, :, pl.ds(to[b] * nb, nb)], buf_b.at[t, q, me[b]], 1, t, q, to)
            local(buf_a.at[t, q, :, pl.ds(me[b] * nb, nb)], buf_b.at[t, q, me[b]], 1, t, q)

    def days(t, q):
        return jnp.concatenate(
            [buf_b[t, q, :, :, n].reshape(256, 128) for n in range(nb)], axis=1
        )

    def send_c(q):
        for t in range(3):
            _, _, c = axes(t)
            arrive(buf_b.at[t, q], 1, t, q)
            sums = dot3(base_t[t], days(t, q))
            for j in range(4):
                for n in range(nb):
                    part[t, q, j, n] = sums[PART * j : PART * (j + 1), 128 * n : 128 * (n + 1)]
            for step in (1, 3, 2):
                to = peer(me, c, step)
                remote(part.at[t, q, to[c]], got.at[t, q, step - 1], 2, t, q, to)

    def send_back_c(q):
        for t in range(3):
            _, _, c = axes(t)
            arrive(got.at[t, q], 2, t, q)
            total = (part[t, q, me[c]] + got[t, q, 0]) + (got[t, q, 1] + got[t, q, 2])
            climate[t, q, me[c]] = total / counts[me[c]][None]
            for step in (1, 3, 2):
                to = peer(me, c, step)
                remote(climate.at[t, q, me[c]], climate.at[t, q, me[c]], 3, t, q, to)

    def send_back_b(q):
        for t in range(3):
            _, b, _ = axes(t)
            arrive(climate.at[t, q, pl.ds(0, 3)], 3, t, q)
            rows = jnp.concatenate(
                [climate[t, q, :, n].reshape(ROWS, 128) for n in range(nb)], axis=1
            )
            rows = jnp.concatenate([rows, jnp.zeros((128 - ROWS, 128 * nb), F32)], axis=0)
            chosen = dot3(member[t], rows)
            for n in range(nb):
                buf_y[t, q, :, :, n] = buf_b[t, q, :, :, n] - chosen[:, 128 * n : 128 * (n + 1)].reshape(4, 8, 8, 128)
            for step in (1, 3, 2):
                to = peer(me, b, step)
                remote(buf_y.at[t, q, to[b]], buf_z.at[t, q, :, pl.ds(me[b] * nb, nb)], 4, t, q, to)
            local(buf_y.at[t, q, me[b]], buf_z.at[t, q, :, pl.ds(me[b] * nb, nb)], 4, t, q)

    def send_back_a(q):
        for t in range(3):
            arrive(buf_z.at[t, q], 4, t, q)
            mine = me[t] * 2 + me[3]
            here = out_ref.at[pl.ds(t * tiles + q * chunk + mine * na, na)]
            for step, core in order:
                to = peer(me, t, step, core)
                remote(buf_z.at[t, q, to[t] * 2 + to[3]], here, 5, t, q, to)
            local(buf_z.at[t, q, mine], here, 5, t, q)

    def finish(q):
        for t in range(3):
            arrive(out_ref.at[pl.ds(t * tiles + q * chunk, chunk)], 5, t, q)

    def prepare():
        load_bucket.wait()
        load_year.wait()
        group = lax.broadcasted_iota(jnp.int32, (HALF, 128), 0)
        seen = jnp.zeros((HALF, 128), F32)
        for r in range(4):
            days_row = jnp.where(year_row[r : r + 1] < BASE_YEARS, bucket_row[r : r + 1], -1)
            seen = seen + jnp.where(days_row == group, 1.0, 0.0)
        number = jnp.maximum(jnp.sum(seen, axis=1, keepdims=True), 1.0)
        number = jnp.broadcast_to(number, (HALF, 128))
        for j in range(4):
            at = (j % 2) * PART
            counts[j] = number[at : at + PART]
        sub = lax.broadcasted_iota(jnp.int32, (8, 128), 0)
        lane = lax.broadcasted_iota(jnp.int32, (8, 128), 1)
        day, column = lax.rem(sub, 4), lane - lax.div(sub, 4) * HALF
        for t in range(3):
            a, b, c = axes(t)

            rows, base_rows = [], []
            for i in range(32):
                at = list(me)
                at[a], at[b], at[3] = (i // 2) % 4, i // 8, i % 2
                tm, space = device(*at)
                first = (tm * 16 + space) * 4
                every = [bucket[first + d] for d in range(4)]
                based = [jnp.where(year[first + d] < BASE_YEARS, every[d], -1000) for d in range(4)]
                pick = lambda v: jnp.where(day == 0, v[0], jnp.where(day == 1, v[1], jnp.where(day == 2, v[2], v[3])))
                rows.append(jnp.where(pick(every) == column, 1.0, 0.0))
                base_rows.append(jnp.where(pick(based) == column, 1.0, 0.0))
            member[t] = jnp.concatenate(rows, axis=0).astype(BF16)
            base_t[t] = jnp.concatenate(base_rows, axis=0).T[:ROWS].astype(BF16)

    stages = (send_a, send_b, send_c, send_back_c, send_back_b, send_back_a, finish)
    send_a(0)
    send_a(1)
    prepare()
    for step in range(1, Q + len(stages) - 1):
        for k in reversed(range(len(stages))):
            q = step - k if k else step + 1
            if 0 <= q < Q:
                stages[k](q)

    for stage, ref in ((0, buf_a), (1, buf_b), (4, buf_z), (5, buf_z)):
        for t in range(3):
            for q in range(Q):
                dims = 7 if stage in (0, 5) else 3
                if stage == 1:
                    piece = ref.at[t, q, pl.ds(0, 3)]
                elif stage == 4:
                    piece = buf_b.at[t, q, pl.ds(0, 3)]
                else:
                    piece = ref.at[t, q, pl.ds(0, dims)]
                pltpu.make_async_copy(piece, piece, sent.at[stage]).wait()
    for stage in (2, 3):
        pltpu.make_async_copy(got, got, sent.at[stage]).wait()


def shards(thermal_field, seasonal_bucket, season_of_record):
    days_here, cells = thermal_field.shape
    blocks = cells // 128
    x = thermal_field.reshape(days_here, blocks, 128).transpose(1, 0, 2)
    x = x.reshape(blocks // 2, 2 * days_here, 128)
    tiles = blocks // 2 // 3
    na, nb = tiles // Q // 8, tiles // Q // 32
    hbm, vmem = pl.BlockSpec(memory_space=pl.ANY), pl.BlockSpec(memory_space=pltpu.VMEM)
    out = pl.pallas_call(
        kernel,
        out_shape=jax.ShapeDtypeStruct(x.shape, F32),
        in_specs=[hbm, vmem, vmem, hbm, hbm],
        out_specs=hbm,
        scratch_shapes=[
            pltpu.VMEM((3, Q, 8, na, 8, 128), F32),
            pltpu.VMEM((3, Q, 4, 8, nb, 8, 128), F32),
            pltpu.VMEM((3, Q, 4, nb, PART, 128), F32),
            pltpu.VMEM((3, Q, 3, nb, PART, 128), F32),
            pltpu.VMEM((3, Q, 4, nb, PART, 128), F32),
            pltpu.VMEM((3, Q, 4, 8, nb, 8, 128), F32),
            pltpu.VMEM((3, Q, 8, na, 8, 128), F32),
            pltpu.VMEM((3, 256, 128), BF16),
            pltpu.VMEM((3, ROWS, 256), BF16),
            pltpu.VMEM((4, PART, 128), F32),
            pltpu.SMEM((512,), jnp.int32),
            pltpu.SMEM((512,), jnp.int32),
            pltpu.SemaphoreType.DMA((6, 3, Q)),
            pltpu.SemaphoreType.DMA((6,)),
            pltpu.SemaphoreType.DMA((2,)),
        ],
        compiler_params=pltpu.CompilerParams(
            collective_id=0, has_side_effects=True, vmem_limit_bytes=60 * 1024 * 1024
        ),
    )(
        x,
        seasonal_bucket.reshape(4, 128),
        season_of_record.reshape(4, 128),
        seasonal_bucket,
        season_of_record,
    )
    out = out.reshape(blocks, days_here, 128).transpose(1, 0, 2)
    return out.reshape(days_here, cells)


def solution(mesh):
    placed = (P(("tm", "space"), None), P(), P())
    return jax.shard_map(
        shards, mesh=mesh, in_specs=placed, out_specs=P(("tm", "space"), None), check_vma=False
    )
```

```python
import functools

import jax
import jax.numpy as jnp
from jax import lax
from jax.experimental import pallas as pl
from jax.experimental.pallas import tpu as pltpu
from jax.sharding import PartitionSpec as P

GROUPS = 46
BASE_YEARS = 6
MESH = pl.DeviceIdType.MESH
F32, BF16 = jnp.float32, jnp.bfloat16

Q = 4
HALF = 48
ROWS = 2 * HALF
PART = ROWS // 4


def coordinates():
    tm, space = lax.axis_index("tm"), lax.axis_index("space")
    x = lax.rem(lax.div(space, 2), 2) * 2 + lax.div(tm, 4)
    return (x, lax.rem(tm, 4), lax.div(space, 4), lax.rem(space, 2))


def device(x, y, z, core):
    return (lax.rem(x, 2) * 4 + y, z * 4 + lax.div(x, 2) * 2 + core)


def peer(me, axis, step, core_step=0):
    at = list(me)
    at[axis] = lax.rem(me[axis] + step, 4)
    at[3] = lax.rem(me[3] + core_step, 2)
    return at


def split(v):
    high = v.astype(BF16)
    rest = v - high.astype(F32)
    middle = rest.astype(BF16)
    low = (rest - middle.astype(F32)).astype(BF16)
    return high, middle, low


def dot3(one_hot, v):
    high, middle, low = split(v)
    dot = functools.partial(jnp.dot, preferred_element_type=F32)
    return dot(one_hot, high) + (dot(one_hot, middle) + dot(one_hot, low))


def kernel(
    x_ref, bucket_row, year_row, bucket_hbm, year_hbm, out_ref,
    buf_a, buf_b, part, got, climate, buf_y, buf_z, member, base_t, counts,
    bucket, year, recv, sent, small,
):
    me = coordinates()
    tiles = x_ref.shape[0] // 3
    chunk = tiles // Q
    na, nb = chunk // 8, chunk // 32

    load_bucket = pltpu.make_async_copy(bucket_hbm, bucket, small.at[0])
    load_year = pltpu.make_async_copy(year_hbm, year, small.at[1])
    load_bucket.start()
    load_year.start()

    barrier = pltpu.get_barrier_semaphore()
    partners = 0
    for axis in range(3):
        for step in range(1, 4):
            for core in range(2):
                pl.semaphore_signal(barrier, inc=1, device_id=device(*peer(me, axis, step, core)), device_id_type=MESH)
                partners += 1
    pl.semaphore_signal(barrier, inc=1, device_id=device(*peer(me, 0, 0, 1)), device_id_type=MESH)
    pl.semaphore_wait(barrier, partners + 1)

    def remote(src, dst, stage, t, q, to):
        pltpu.make_async_remote_copy(
            src_ref=src, dst_ref=dst, send_sem=sent.at[stage], recv_sem=recv.at[stage, t, q],
            device_id=device(*to), device_id_type=MESH,
        ).start()

    def local(src, dst, stage, t, q):
        pltpu.make_async_copy(src, dst, recv.at[stage, t, q]).start()

    def arrive(ref, stage, t, q):
        pltpu.make_async_copy(ref, ref, recv.at[stage, t, q]).wait()

    def axes(t):
        return t, (t + 1) % 3, (t + 2) % 3

    order = ((1, 0), (3, 0), (2, 0), (1, 1), (3, 1), (2, 1), (0, 1))

    def send_a(q):
        for t in range(3):
            mine = me[t] * 2 + me[3]
            local(x_ref.at[pl.ds(t * tiles + q * chunk + mine * na, na)], buf_a.at[t, q, mine], 0, t, q)
        for step, core in order:
            for t in range(3):
                to = peer(me, t, step, core)
                mine, theirs = me[t] * 2 + me[3], to[t] * 2 + to[3]
                remote(x_ref.at[pl.ds(t * tiles + q * chunk + theirs * na, na)], buf_a.at[t, q, mine], 0, t, q, to)

    def send_b(q):
        for t in range(3):
            _, b, _ = axes(t)
            arrive(buf_a.at[t, q], 0, t, q)
            for step in (1, 3, 2):
                to = peer(me, b, step)
                remote(buf_a.at[t, q, :, pl.ds(to[b] * nb, nb)], buf_b.at[t, q, me[b]], 1, t, q, to)
            local(buf_a.at[t, q, :, pl.ds(me[b] * nb, nb)], buf_b.at[t, q, me[b]], 1, t, q)

    def days(t, q):
        return jnp.concatenate(
            [buf_b[t, q, :, :, n].reshape(256, 128) for n in range(nb)], axis=1
        )

    def send_c(q):
        for t in range(3):
            _, _, c = axes(t)
            arrive(buf_b.at[t, q], 1, t, q)
            sums = dot3(base_t[t], days(t, q))
            for j in range(4):
                for n in range(nb):
                    part[t, q, j, n] = sums[PART * j : PART * (j + 1), 128 * n : 128 * (n + 1)]
            for step in (1, 3, 2):
                to = peer(me, c, step)
                remote(part.at[t, q, to[c]], got.at[t, q, step - 1], 2, t, q, to)

    def send_back_c(q):
        for t in range(3):
            _, _, c = axes(t)
            arrive(got.at[t, q], 2, t, q)
            total = (part[t, q, me[c]] + got[t, q, 0]) + (got[t, q, 1] + got[t, q, 2])
            climate[t, q, me[c]] = total / counts[me[c]][None]
            for step in (1, 3, 2):
                to = peer(me, c, step)
                remote(climate.at[t, q, me[c]], climate.at[t, q, me[c]], 3, t, q, to)

    def send_back_b(q):
        for t in range(3):
            _, b, _ = axes(t)
            arrive(climate.at[t, q, pl.ds(0, 3)], 3, t, q)
            rows = jnp.concatenate(
                [climate[t, q, :, n].reshape(ROWS, 128) for n in range(nb)], axis=1
            )
            rows = jnp.concatenate([rows, jnp.zeros((128 - ROWS, 128 * nb), F32)], axis=0)
            chosen = dot3(member[t], rows)
            for n in range(nb):
                buf_y[t, q, :, :, n] = buf_b[t, q, :, :, n] - chosen[:, 128 * n : 128 * (n + 1)].reshape(4, 8, 8, 128)
            for step in (1, 3, 2):
                to = peer(me, b, step)
                remote(buf_y.at[t, q, to[b]], buf_z.at[t, q, :, pl.ds(me[b] * nb, nb)], 4, t, q, to)
            local(buf_y.at[t, q, me[b]], buf_z.at[t, q, :, pl.ds(me[b] * nb, nb)], 4, t, q)

    def send_back_a(q):
        for t in range(3):
            arrive(buf_z.at[t, q], 4, t, q)
            mine = me[t] * 2 + me[3]
            here = out_ref.at[pl.ds(t * tiles + q * chunk + mine * na, na)]
            for step, core in order:
                to = peer(me, t, step, core)
                remote(buf_z.at[t, q, to[t] * 2 + to[3]], here, 5, t, q, to)
            local(buf_z.at[t, q, mine], here, 5, t, q)

    def finish(q):
        for t in range(3):
            arrive(out_ref.at[pl.ds(t * tiles + q * chunk, chunk)], 5, t, q)

    def prepare():
        load_bucket.wait()
        load_year.wait()
        group = lax.broadcasted_iota(jnp.int32, (HALF, 128), 0)
        seen = jnp.zeros((HALF, 128), F32)
        for r in range(4):
            days_row = jnp.where(year_row[r : r + 1] < BASE_YEARS, bucket_row[r : r + 1], -1)
            seen = seen + jnp.where(days_row == group, 1.0, 0.0)
        number = jnp.maximum(jnp.sum(seen, axis=1, keepdims=True), 1.0)
        number = jnp.broadcast_to(number, (HALF, 128))
        for j in range(4):
            at = (j % 2) * PART
            counts[j] = number[at : at + PART]
        sub = lax.broadcasted_iota(jnp.int32, (8, 128), 0)
        lane = lax.broadcasted_iota(jnp.int32, (8, 128), 1)
        day, column = lax.rem(sub, 4), lane - lax.div(sub, 4) * HALF
        for t in range(3):
            a, b, c = axes(t)

            rows, base_rows = [], []
            for i in range(32):
                at = list(me)
                at[a], at[b], at[3] = (i // 2) % 4, i // 8, i % 2
                tm, space = device(*at)
                first = (tm * 16 + space) * 4
                every = [bucket[first + d] for d in range(4)]
                based = [jnp.where(year[first + d] < BASE_YEARS, every[d], -1000) for d in range(4)]
                pick = lambda v: jnp.where(day == 0, v[0], jnp.where(day == 1, v[1], jnp.where(day == 2, v[2], v[3])))
                rows.append(jnp.where(pick(every) == column, 1.0, 0.0))
                base_rows.append(jnp.where(pick(based) == column, 1.0, 0.0))
            member[t] = jnp.concatenate(rows, axis=0).astype(BF16)
            base_t[t] = jnp.concatenate(base_rows, axis=0).T[:ROWS].astype(BF16)

    stages = (send_a, send_b, send_c, send_back_c, send_back_b, send_back_a)
    send_a(0)
    send_a(1)
    prepare()
    for step in range(1, Q + len(stages)):
        for k in range(len(stages)):
            q = step - k if k else step + 1
            if 0 <= q < Q:
                stages[k](q)
    for q in range(Q):
        finish(q)

    for stage, ref in ((0, buf_a), (1, buf_b), (4, buf_z), (5, buf_z)):
        for t in range(3):
            for q in range(Q):
                dims = 7 if stage in (0, 5) else 3
                if stage == 1:
                    piece = ref.at[t, q, pl.ds(0, 3)]
                elif stage == 4:
                    piece = buf_b.at[t, q, pl.ds(0, 3)]
                else:
                    piece = ref.at[t, q, pl.ds(0, dims)]
                pltpu.make_async_copy(piece, piece, sent.at[stage]).wait()
    for stage in (2, 3):
        pltpu.make_async_copy(got, got, sent.at[stage]).wait()


def shards(thermal_field, seasonal_bucket, season_of_record):
    days_here, cells = thermal_field.shape
    blocks = cells // 128
    x = thermal_field.reshape(days_here, blocks, 128).transpose(1, 0, 2)
    x = x.reshape(blocks // 2, 2 * days_here, 128)
    tiles = blocks // 2 // 3
    na, nb = tiles // Q // 8, tiles // Q // 32
    hbm, vmem = pl.BlockSpec(memory_space=pl.ANY), pl.BlockSpec(memory_space=pltpu.VMEM)
    out = pl.pallas_call(
        kernel,
        out_shape=pltpu.VMEM(x.shape, F32),
        in_specs=[hbm, vmem, vmem, hbm, hbm],
        out_specs=hbm,
        scratch_shapes=[
            pltpu.VMEM((3, Q, 8, na, 8, 128), F32),
            pltpu.VMEM((3, Q, 4, 8, nb, 8, 128), F32),
            pltpu.VMEM((3, Q, 4, nb, PART, 128), F32),
            pltpu.VMEM((3, Q, 3, nb, PART, 128), F32),
            pltpu.VMEM((3, Q, 4, nb, PART, 128), F32),
            pltpu.VMEM((3, Q, 4, 8, nb, 8, 128), F32),
            pltpu.VMEM((3, Q, 8, na, 8, 128), F32),
            pltpu.VMEM((3, 256, 128), BF16),
            pltpu.VMEM((3, ROWS, 256), BF16),
            pltpu.VMEM((4, PART, 128), F32),
            pltpu.SMEM((512,), jnp.int32),
            pltpu.SMEM((512,), jnp.int32),
            pltpu.SemaphoreType.DMA((6, 3, Q)),
            pltpu.SemaphoreType.DMA((6,)),
            pltpu.SemaphoreType.DMA((2,)),
        ],
        compiler_params=pltpu.CompilerParams(
            collective_id=0, has_side_effects=True, vmem_limit_bytes=63_880_000
        ),
    )(
        x,
        seasonal_bucket.reshape(4, 128),
        season_of_record.reshape(4, 128),
        seasonal_bucket,
        season_of_record,
    )
    out = out.reshape(blocks, days_here, 128).transpose(1, 0, 2)
    return out.reshape(days_here, cells)


def solution(mesh):
    placed = (P(("tm", "space"), None), P(), P())
    return jax.shard_map(
        shards, mesh=mesh, in_specs=placed, out_specs=P(("tm", "space"), None), check_vma=False
    )
```

```python
import functools

import jax
import jax.numpy as jnp
from jax import lax
from jax.experimental import pallas as pl
from jax.experimental.pallas import tpu as pltpu
from jax.sharding import PartitionSpec as P

GROUPS = 46
BASE_YEARS = 6
MIDDLE = 250.0
MESH = pl.DeviceIdType.MESH
F32, BF16 = jnp.float32, jnp.bfloat16

Q = 4
HALF = 48
ROWS = 2 * HALF
PART = ROWS // 4


def coordinates():
    tm, space = lax.axis_index("tm"), lax.axis_index("space")
    x = lax.rem(lax.div(space, 2), 2) * 2 + lax.div(tm, 4)
    return (x, lax.rem(tm, 4), lax.div(space, 4), lax.rem(space, 2))


def device(x, y, z, core):
    return (lax.rem(x, 2) * 4 + y, z * 4 + lax.div(x, 2) * 2 + core)


def peer(me, axis, step, core_step=0):
    at = list(me)
    at[axis] = lax.rem(me[axis] + step, 4)
    at[3] = lax.rem(me[3] + core_step, 2)
    return at


def dot2(one_hot_twice, v):
    high = v.astype(BF16)
    low = (v - high.astype(F32)).astype(BF16)
    return jnp.dot(one_hot_twice, jnp.concatenate([high, low], axis=0), preferred_element_type=F32)


def halving(at, axis, h):
    m = at[axis]
    up = lax.rem(m + h, 2) == 0
    one, two = jnp.where(up, 1, 3), jnp.where(up, 3, 1)
    u = lax.rem(lax.div(m + 1 - h, 2), 2)
    v = lax.rem(m, 2) if h else lax.div(m, 2)
    return peer(at, axis, one), peer(at, axis, two), u, v


def kernel(
    x_ref, bucket_rows, year_rows, bucket_hbm, year_hbm, out_ref,
    buf_a, buf_b, part, kept, got_b, got_c, mean, got_e, buf_y, buf_z,
    member, base_t, counts, bucket_row, year_row, bucket, year, recv, sent, small,
):
    me = coordinates()
    tiles = x_ref.shape[0] // 3
    chunk = tiles // Q
    na = chunk // 8
    nh, nu, nv = na // 2, na // 4, na // 8

    loads = [
        pltpu.make_async_copy(src, dst, small.at[i])
        for i, (src, dst) in enumerate(
            ((bucket_hbm, bucket), (year_hbm, year), (bucket_rows, bucket_row), (year_rows, year_row))
        )
    ]
    for load in loads:
        load.start()

    barrier = pltpu.get_barrier_semaphore()
    partners = 0
    for axis in range(3):
        for step in range(1, 4):
            for core in range(2):
                pl.semaphore_signal(barrier, inc=1, device_id=device(*peer(me, axis, step, core)), device_id_type=MESH)
                partners += 1
    pl.semaphore_signal(barrier, inc=1, device_id=device(*peer(me, 0, 0, 1)), device_id_type=MESH)
    pl.semaphore_wait(barrier, partners + 1)

    def remote(src, dst, stage, t, q, h, to):
        pltpu.make_async_remote_copy(
            src_ref=src, dst_ref=dst, send_sem=sent.at[stage], recv_sem=recv.at[stage, t, q, h],
            device_id=device(*to), device_id_type=MESH,
        ).start()

    def local(src, dst, stage, t, q):
        pltpu.make_async_copy(src, dst, recv.at[stage, t, q, 0]).start()

    def arrive(ref, stage, t, q, h=0):
        pltpu.make_async_copy(ref, ref, recv.at[stage, t, q, h]).wait()

    def axes(t):
        return t, (t + 1) % 3, (t + 2) % 3

    order = ((1, 0), (3, 0), (2, 0), (1, 1), (3, 1), (2, 1), (0, 1))
    pairs = [(t, h) for t in range(3) for h in range(2)]

    def send_a(q):
        for t in range(3):
            mine = me[t] * 2 + me[3]
            local(x_ref.at[pl.ds(t * tiles + q * chunk + mine * na, na)], buf_a.at[t, q, mine], 0, t, q)
        for step, core in order:
            for t in range(3):
                to = peer(me, t, step, core)
                mine, theirs = me[t] * 2 + me[3], to[t] * 2 + to[3]
                remote(x_ref.at[pl.ds(t * tiles + q * chunk + theirs * na, na)], buf_a.at[t, q, mine], 0, t, q, 0, to)

    def send_b1(q):
        for t, h in pairs:
            if h == 0:
                arrive(buf_a.at[t, q], 0, t, q)
            one, _, u, _ = halving(me, axes(t)[1], h)
            remote(buf_a.at[t, q, :, pl.ds(h * nh + (1 - u) * nu, nu)], buf_b.at[t, q, h], 1, t, q, h, one)

    def send_b2(q):
        for t in range(3):
            sums = []
            for h in range(2):
                _, _, u, v = halving(me, axes(t)[1], h)
                arrive(buf_b.at[t, q, h], 1, t, q, h)
                columns = []
                for half in (1 - v, v):
                    for n in range(nv):
                        k = half * nv + n
                        mine = buf_a[t, q, :, h * nh + u * nu + k].reshape(64, 128)
                        theirs = buf_b[t, q, h, :, k].reshape(64, 128)
                        columns.append(jnp.concatenate([mine, theirs], axis=0))
                sums.append(dot2(base_t[t, h], jnp.concatenate(columns, axis=1) - MIDDLE))
            for h in range(2):
                for n in range(nv):
                    for j in range(4):
                        rows = slice(PART * j, PART * (j + 1))
                        part[t, q, h, j, n] = sums[h][rows, 128 * n : 128 * (n + 1)]
                        kept[t, q, j, h, n] = sums[h][rows, 128 * (nv + n) : 128 * (nv + n + 1)]
            for h in range(2):
                two = halving(me, axes(t)[1], h)[1]
                remote(part.at[t, q, h], got_b.at[t, q, h], 2, t, q, h, two)

    def send_c(q):
        for t in range(3):
            c = axes(t)[2]
            for h in range(2):
                arrive(got_b.at[t, q, h], 2, t, q, h)
                for j in range(4):
                    kept[t, q, j, h] += got_b[t, q, h, j]
            for step in (1, 3, 2):
                to = peer(me, c, step)
                remote(kept.at[t, q, to[c]], got_c.at[t, q, step - 1], 3, t, q, 0, to)

    def send_d(q):
        for t in range(3):
            c = axes(t)[2]
            arrive(got_c.at[t, q], 3, t, q)
            total = (kept[t, q, me[c]] + got_c[t, q, 0]) + (got_c[t, q, 1] + got_c[t, q, 2])
            mean[t, q, me[c]] = total / counts[me[c]][None, None]
            for step in (1, 3, 2):
                to = peer(me, c, step)
                remote(mean.at[t, q, me[c]], mean.at[t, q, me[c]], 4, t, q, 0, to)

    def send_e2(q):
        for t in range(3):
            arrive(mean.at[t, q, pl.ds(0, 3)], 4, t, q)
            for h in range(2):
                two = halving(me, axes(t)[1], h)[1]
                remote(mean.at[t, q, :, h], got_e.at[t, q, h], 5, t, q, h, two)

    def send_e1(q):
        for t in range(3):
            chosen = []
            for h in range(2):
                arrive(got_e.at[t, q, h], 5, t, q, h)
                rows = jnp.concatenate(
                    [mean[t, q, :, h, n].reshape(ROWS, 128) for n in range(nv)]
                    + [got_e[t, q, h, :, n].reshape(ROWS, 128) for n in range(nv)],
                    axis=1,
                )
                rows = jnp.concatenate([rows, jnp.zeros((128 - ROWS, 128 * nu), F32)], axis=0)
                chosen.append(dot2(member[t, h], rows))
            for h in range(2):
                one, _, u, v = halving(me, axes(t)[1], h)
                at = h * nh + u * nu
                for k in range(nu):
                    to = (v if k < nv else 1 - v) * nv + k % nv
                    column = chosen[h][64:, 128 * k : 128 * (k + 1)]
                    buf_y[t, q, h, :, to] = (buf_b[t, q, h, :, to] - MIDDLE) - column.reshape(8, 8, 128)
                remote(buf_y.at[t, q, h], buf_z.at[t, q, :, pl.ds(at, nu)], 6, t, q, h, one)
            for h in range(2):
                _, _, u, v = halving(me, axes(t)[1], h)
                at = h * nh + u * nu
                for k in range(nu):
                    to = at + (v if k < nv else 1 - v) * nv + k % nv
                    column = chosen[h][:64, 128 * k : 128 * (k + 1)]
                    buf_z[t, q, :, to] = (buf_a[t, q, :, to] - MIDDLE) - column.reshape(8, 8, 128)

    def send_f(q):
        for t in range(3):
            for h in range(2):
                arrive(buf_y.at[t, q, h], 6, t, q, h)
            mine = me[t] * 2 + me[3]
            here = out_ref.at[pl.ds(t * tiles + q * chunk + mine * na, na)]
            for step, core in order:
                to = peer(me, t, step, core)
                remote(buf_z.at[t, q, to[t] * 2 + to[3]], here, 7, t, q, 0, to)
            local(buf_z.at[t, q, mine], here, 7, t, q)

    def finish(q):
        for t in range(3):
            arrive(out_ref.at[pl.ds(t * tiles + q * chunk, chunk)], 7, t, q)

    def prepare():
        for load in loads:
            load.wait()
        group = lax.broadcasted_iota(jnp.int32, (HALF, 128), 0)
        seen = jnp.zeros((HALF, 128), F32)
        for r in range(4):
            days_row = jnp.where(year_row[r : r + 1] < BASE_YEARS, bucket_row[r : r + 1], -1)
            seen = seen + jnp.where(days_row == group, 1.0, 0.0)
        number = jnp.maximum(jnp.sum(seen, axis=1, keepdims=True), 1.0)
        number = jnp.broadcast_to(number, (HALF, 128))
        for j in range(4):
            at = (j % 2) * PART
            counts[j] = number[at : at + PART]
        sub = lax.broadcasted_iota(jnp.int32, (8, 128), 0)
        lane = lax.broadcasted_iota(jnp.int32, (8, 128), 1)
        day, column = lax.rem(sub, 4), lane - lax.div(sub, 4) * HALF

        def pick(v):
            chosen = jnp.where(day == 0, v[0], jnp.where(day == 1, v[1], jnp.where(day == 2, v[2], v[3])))
            return jnp.where(chosen == column, 1.0, 0.0)

        def line(at, a):
            every, based = [], []
            for i in range(8):
                who = list(at)
                who[a], who[3] = i // 2, i % 2
                tm, space = device(*who)
                first = (tm * 16 + space) * 4
                groups = [bucket[first + d] for d in range(4)]
                every.append(pick(groups))
                based.append(pick([jnp.where(year[first + d] < BASE_YEARS, groups[d], -1000) for d in range(4)]))
            return every, based

        for t in range(3):
            a, b, _ = axes(t)
            mine, mine_base = line(me, a)
            for h in range(2):
                theirs, theirs_base = line(halving(me, b, h)[0], a)
                every = jnp.concatenate(mine + theirs, axis=0).astype(BF16)
                based = jnp.concatenate(mine_base + theirs_base, axis=0).T[:ROWS].astype(BF16)
                member[t, h] = jnp.concatenate([every, every], axis=1)
                base_t[t, h] = jnp.concatenate([based, based], axis=1)

    stages = (send_a, send_b1, send_b2, send_c, send_d, send_e2, send_e1, send_f)
    stages[0](0)
    stages[0](1)
    stages[0](2)
    stages[0](3)
    prepare()
    stages[1](0)
    stages[1](1)
    stages[1](2)
    stages[1](3)
    stages[2](0)
    stages[2](1)
    stages[2](2)
    stages[2](3)
    stages[3](0)
    stages[3](1)
    stages[3](2)
    stages[3](3)
    stages[4](0)
    stages[4](1)
    stages[4](2)
    stages[4](3)
    stages[5](0)
    stages[5](1)
    stages[5](2)
    stages[5](3)
    stages[6](0)
    stages[6](1)
    stages[6](2)
    stages[6](3)
    stages[7](0)
    stages[7](1)
    stages[7](2)
    stages[7](3)
    for q in range(Q):
        finish(q)

    for stage, ref in ((0, buf_a), (7, buf_z)):
        for t in range(3):
            for q in range(Q):
                piece = ref.at[t, q, pl.ds(0, 7)]
                pltpu.make_async_copy(piece, piece, sent.at[stage]).wait()
    for stage, ref in ((1, buf_b), (2, got_b), (3, got_c), (4, got_c), (5, got_e), (6, buf_b)):
        pltpu.make_async_copy(ref, ref, sent.at[stage]).wait()


def shards(thermal_field, seasonal_bucket, season_of_record):
    days_here, cells = thermal_field.shape
    blocks = cells // 128
    x = thermal_field.reshape(days_here, blocks, 128).transpose(1, 0, 2)
    x = x.reshape(blocks // 2, 2 * days_here, 128)
    tiles = blocks // 2 // 3
    na, nv = tiles // Q // 8, tiles // Q // 64
    hbm = pl.BlockSpec(memory_space=pl.ANY)
    out = pl.pallas_call(
        kernel,
        out_shape=pltpu.VMEM(x.shape, F32),
        in_specs=[hbm] * 5,
        out_specs=hbm,
        scratch_shapes=[
            pltpu.VMEM((3, Q, 8, na, 8, 128), F32),
            pltpu.VMEM((3, Q, 2, 8, na // 4, 8, 128), F32),
            pltpu.VMEM((3, Q, 2, 4, nv, PART, 128), F32),
            pltpu.VMEM((3, Q, 4, 2, nv, PART, 128), F32),
            pltpu.VMEM((3, Q, 2, 4, nv, PART, 128), F32),
            pltpu.VMEM((3, Q, 3, 2, nv, PART, 128), F32),
            pltpu.VMEM((3, Q, 4, 2, nv, PART, 128), F32),
            pltpu.VMEM((3, Q, 2, 4, nv, PART, 128), F32),
            pltpu.VMEM((3, Q, 2, 8, na // 4, 8, 128), F32),
            pltpu.VMEM((3, Q, 8, na, 8, 128), F32),
            pltpu.VMEM((3, 2, 128, 256), BF16),
            pltpu.VMEM((3, 2, ROWS, 256), BF16),
            pltpu.VMEM((4, PART, 128), F32),
            pltpu.VMEM((4, 128), jnp.int32),
            pltpu.VMEM((4, 128), jnp.int32),
            pltpu.SMEM((512,), jnp.int32),
            pltpu.SMEM((512,), jnp.int32),
            pltpu.SemaphoreType.DMA((8, 3, Q, 2)),
            pltpu.SemaphoreType.DMA((8,)),
            pltpu.SemaphoreType.DMA((4,)),
        ],
        compiler_params=pltpu.CompilerParams(
            collective_id=0, has_side_effects=True, vmem_limit_bytes=63_880_000
        ),
    )(
        x,
        seasonal_bucket.reshape(4, 128),
        season_of_record.reshape(4, 128),
        seasonal_bucket,
        season_of_record,
    )
    out = out.reshape(blocks, days_here, 128).transpose(1, 0, 2)
    return out.reshape(days_here, cells)


def solution(mesh):
    placed = (P(("tm", "space"), None), P(), P())
    return jax.shard_map(
        shards, mesh=mesh, in_specs=placed, out_specs=P(("tm", "space"), None), check_vma=False
    )
```

```python
import functools

import jax
import jax.numpy as jnp
from jax import lax
from jax.experimental import pallas as pl
from jax.experimental.pallas import tpu as pltpu
from jax.sharding import PartitionSpec as P

GROUPS = 46
BASE_YEARS = 6
MIDDLE = 250.0
MESH = pl.DeviceIdType.MESH
F32, BF16 = jnp.float32, jnp.bfloat16

Q = 4
HALF = 48
ROWS = 2 * HALF
PART = ROWS // 4
REAL = GROUPS // 2


def coordinates():
    tm, space = lax.axis_index("tm"), lax.axis_index("space")
    x = lax.rem(lax.div(space, 2), 2) * 2 + lax.div(tm, 4)
    return (x, lax.rem(tm, 4), lax.div(space, 4), lax.rem(space, 2))


def device(x, y, z, core):
    return (lax.rem(x, 2) * 4 + y, z * 4 + lax.div(x, 2) * 2 + core)


def peer(me, axis, step, core_step=0):
    at = list(me)
    at[axis] = lax.rem(me[axis] + step, 4)
    at[3] = lax.rem(me[3] + core_step, 2)
    return at


def dot2(one_hot_twice, v):
    high = v.astype(BF16)
    low = (v - high.astype(F32)).astype(BF16)
    return jnp.dot(one_hot_twice, jnp.concatenate([high, low], axis=0), preferred_element_type=F32)


def halving(at, axis, h):
    m = at[axis]
    up = lax.rem(m + h, 2) == 0
    one, two = jnp.where(up, 1, 3), jnp.where(up, 3, 1)
    u = lax.rem(lax.div(m + 1 - h, 2), 2)
    v = lax.rem(m, 2) if h else lax.div(m, 2)
    return peer(at, axis, one), peer(at, axis, two), u, v


def kernel(
    x_ref, bucket_rows, year_rows, bucket_hbm, year_hbm, out_ref,
    buf_a, buf_b, part, kept, got_b, got_c, mean, got_e, buf_y, buf_z,
    member, base_t, counts, bucket_row, year_row, bucket, year, recv, sent, small,
):
    me = coordinates()
    tiles = x_ref.shape[0] // 3
    chunk = tiles // Q
    na = chunk // 8
    nh, nu, nv = na // 2, na // 4, na // 8

    loads = [
        pltpu.make_async_copy(src, dst, small.at[i])
        for i, (src, dst) in enumerate(
            ((bucket_hbm, bucket), (year_hbm, year), (bucket_rows, bucket_row), (year_rows, year_row))
        )
    ]
    for load in loads:
        load.start()

    barrier = pltpu.get_barrier_semaphore()
    partners = 0
    for axis in range(3):
        for step in range(1, 4):
            for core in range(2):
                pl.semaphore_signal(barrier, inc=1, device_id=device(*peer(me, axis, step, core)), device_id_type=MESH)
                partners += 1
    pl.semaphore_signal(barrier, inc=1, device_id=device(*peer(me, 0, 0, 1)), device_id_type=MESH)
    pl.semaphore_wait(barrier, partners + 1)

    def remote(src, dst, stage, t, q, h, to):
        pltpu.make_async_remote_copy(
            src_ref=src, dst_ref=dst, send_sem=sent.at[stage], recv_sem=recv.at[stage, t, q, h],
            device_id=device(*to), device_id_type=MESH,
        ).start()

    def local(src, dst, stage, t, q):
        pltpu.make_async_copy(src, dst, recv.at[stage, t, q, 0]).start()

    def arrive(ref, stage, t, q, h=0):
        pltpu.make_async_copy(ref, ref, recv.at[stage, t, q, h]).wait()

    def axes(t):
        return t, (t + 1) % 3, (t + 2) % 3

    order = ((1, 0), (3, 0), (2, 0), (1, 1), (3, 1), (2, 1), (0, 1))
    real = pl.ds(0, REAL)
    row = lax.broadcasted_iota(jnp.int32, (4, PART, 128), 1)
    pairs = [(t, h) for t in range(3) for h in range(2)]

    def send_a(q):
        for t in range(3):
            mine = me[t] * 2 + me[3]
            local(x_ref.at[pl.ds(t * tiles + q * chunk + mine * na, na)], buf_a.at[t, q, mine], 0, t, q)
        for step, core in order:
            for t in range(3):
                to = peer(me, t, step, core)
                mine, theirs = me[t] * 2 + me[3], to[t] * 2 + to[3]
                remote(x_ref.at[pl.ds(t * tiles + q * chunk + theirs * na, na)], buf_a.at[t, q, mine], 0, t, q, 0, to)

    def send_b1(q):
        for t, h in pairs:
            if h == 0:
                arrive(buf_a.at[t, q], 0, t, q)
            one, _, u, _ = halving(me, axes(t)[1], h)
            remote(buf_a.at[t, q, :, pl.ds(h * nh + (1 - u) * nu, nu)], buf_b.at[t, q, h], 1, t, q, h, one)

    def send_b2(q):
        for t in range(3):
            sums = []
            for h in range(2):
                _, _, u, v = halving(me, axes(t)[1], h)
                arrive(buf_b.at[t, q, h], 1, t, q, h)
                columns = []
                for half in (1 - v, v):
                    for n in range(nv):
                        k = half * nv + n
                        mine = buf_a[t, q, :, h * nh + u * nu + k].reshape(64, 128)
                        theirs = buf_b[t, q, h, :, k].reshape(64, 128)
                        columns.append(jnp.concatenate([mine, theirs], axis=0))
                sums.append(dot2(base_t[t, h], jnp.concatenate(columns, axis=1) - MIDDLE))
            for h in range(2):
                for n in range(nv):
                    for j in range(4):
                        rows = slice(PART * j, PART * (j + 1))
                        part[t, q, h, j, n] = sums[h][rows, 128 * n : 128 * (n + 1)]
                        kept[t, q, j, h, n] = sums[h][rows, 128 * (nv + n) : 128 * (nv + n + 1)]
            for h in range(2):
                two = halving(me, axes(t)[1], h)[1]
                remote(part.at[t, q, h, :, :, real], got_b.at[t, q, h, :, :, real], 2, t, q, h, two)

    def send_c(q):
        for t in range(3):
            c = axes(t)[2]
            for h in range(2):
                arrive(got_b.at[t, q, h, :, :, real], 2, t, q, h)
                for j in range(4):
                    kept[t, q, j, h] += got_b[t, q, h, j]
            for step in (1, 3, 2):
                to = peer(me, c, step)
                remote(kept.at[t, q, to[c], :, :, real], got_c.at[t, q, step - 1, :, :, real], 3, t, q, 0, to)

    def send_d(q):
        for t in range(3):
            c = axes(t)[2]
            arrive(got_c.at[t, q, :, :, :, real], 3, t, q)
            total = (kept[t, q, me[c]] + got_c[t, q, 0]) + (got_c[t, q, 1] + got_c[t, q, 2])
            mean[t, q, me[c]] = total / counts[me[c]][None, None]
            for step in (1, 3, 2):
                to = peer(me, c, step)
                remote(mean.at[t, q, me[c], :, :, real], mean.at[t, q, me[c], :, :, real], 4, t, q, 0, to)

    def send_e2(q):
        for t in range(3):
            arrive(mean.at[t, q, pl.ds(0, 3), :, :, real], 4, t, q)
            for h in range(2):
                two = halving(me, axes(t)[1], h)[1]
                remote(mean.at[t, q, :, h, :, real], got_e.at[t, q, h, :, :, real], 5, t, q, h, two)

    def send_e1(q):
        for t in range(3):
            chosen = []
            for h in range(2):
                arrive(got_e.at[t, q, h, :, :, real], 5, t, q, h)
                rows = jnp.concatenate(
                    [jnp.where(row < REAL, mean[t, q, :, h, n], 0.0).reshape(ROWS, 128) for n in range(nv)]
                    + [jnp.where(row < REAL, got_e[t, q, h, :, n], 0.0).reshape(ROWS, 128) for n in range(nv)],
                    axis=1,
                )
                rows = jnp.concatenate([rows, jnp.zeros((128 - ROWS, 128 * nu), F32)], axis=0)
                chosen.append(dot2(member[t, h], rows))
            for h in range(2):
                one, _, u, v = halving(me, axes(t)[1], h)
                at = h * nh + u * nu
                for k in range(nu):
                    to = (v if k < nv else 1 - v) * nv + k % nv
                    column = chosen[h][64:, 128 * k : 128 * (k + 1)]
                    buf_y[t, q, h, :, to] = (buf_b[t, q, h, :, to] - MIDDLE) - column.reshape(8, 8, 128)
                remote(buf_y.at[t, q, h], buf_z.at[t, q, :, pl.ds(at, nu)], 6, t, q, h, one)
            for h in range(2):
                _, _, u, v = halving(me, axes(t)[1], h)
                at = h * nh + u * nu
                for k in range(nu):
                    to = at + (v if k < nv else 1 - v) * nv + k % nv
                    column = chosen[h][:64, 128 * k : 128 * (k + 1)]
                    buf_z[t, q, :, to] = (buf_a[t, q, :, to] - MIDDLE) - column.reshape(8, 8, 128)

    def send_f(q):
        for t in range(3):
            for h in range(2):
                arrive(buf_y.at[t, q, h], 6, t, q, h)
            mine = me[t] * 2 + me[3]
            here = out_ref.at[pl.ds(t * tiles + q * chunk + mine * na, na)]
            for step, core in order:
                to = peer(me, t, step, core)
                remote(buf_z.at[t, q, to[t] * 2 + to[3]], here, 7, t, q, 0, to)
            local(buf_z.at[t, q, mine], here, 7, t, q)

    def finish(q):
        for t in range(3):
            arrive(out_ref.at[pl.ds(t * tiles + q * chunk, chunk)], 7, t, q)

    def place(group):
        return group + jnp.where(group < REAL, 0, 1)

    def prepare():
        for load in loads:
            load.wait()
        group = lax.broadcasted_iota(jnp.int32, (HALF, 128), 0)
        seen = jnp.zeros((HALF, 128), F32)
        for r in range(4):
            days_row = jnp.where(year_row[r : r + 1] < BASE_YEARS, place(bucket_row[r : r + 1]), -1)
            seen = seen + jnp.where(days_row == group, 1.0, 0.0)
        number = jnp.maximum(jnp.sum(seen, axis=1, keepdims=True), 1.0)
        number = jnp.broadcast_to(number, (HALF, 128))
        for j in range(4):
            at = (j % 2) * PART
            counts[j] = number[at : at + PART]
        sub = lax.broadcasted_iota(jnp.int32, (8, 128), 0)
        lane = lax.broadcasted_iota(jnp.int32, (8, 128), 1)
        day, column = lax.rem(sub, 4), lane - lax.div(sub, 4) * HALF

        def pick(v):
            chosen = jnp.where(day == 0, v[0], jnp.where(day == 1, v[1], jnp.where(day == 2, v[2], v[3])))
            return jnp.where(chosen == column, 1.0, 0.0)

        def line(at, a):
            every, based = [], []
            for i in range(8):
                who = list(at)
                who[a], who[3] = i // 2, i % 2
                tm, space = device(*who)
                first = (tm * 16 + space) * 4
                groups = [place(bucket[first + d]) for d in range(4)]
                every.append(pick(groups))
                based.append(pick([jnp.where(year[first + d] < BASE_YEARS, groups[d], -1000) for d in range(4)]))
            return every, based

        for t in range(3):
            a, b, _ = axes(t)
            mine, mine_base = line(me, a)
            for h in range(2):
                theirs, theirs_base = line(halving(me, b, h)[0], a)
                every = jnp.concatenate(mine + theirs, axis=0).astype(BF16)
                based = jnp.concatenate(mine_base + theirs_base, axis=0).T[:ROWS].astype(BF16)
                member[t, h] = jnp.concatenate([every, every], axis=1)
                base_t[t, h] = jnp.concatenate([based, based], axis=1)

    stages = (send_a, send_b1, send_b2, send_c, send_d, send_e2, send_e1, send_f)
    stages[0](0)
    stages[0](1)
    stages[0](2)
    stages[0](3)
    prepare()
    stages[1](0)
    stages[1](1)
    stages[1](2)
    stages[1](3)
    stages[2](0)
    stages[2](1)
    stages[2](2)
    stages[2](3)
    stages[3](0)
    stages[3](1)
    stages[3](2)
    stages[3](3)
    stages[4](0)
    stages[4](1)
    stages[4](2)
    stages[4](3)
    stages[5](0)
    stages[5](1)
    stages[5](2)
    stages[5](3)
    stages[6](0)
    stages[6](1)
    stages[6](2)
    stages[6](3)
    stages[7](0)
    stages[7](1)
    stages[7](2)
    stages[7](3)
    for q in range(Q):
        finish(q)

    for stage, ref in ((0, buf_a), (7, buf_z)):
        for t in range(3):
            for q in range(Q):
                piece = ref.at[t, q, pl.ds(0, 7)]
                pltpu.make_async_copy(piece, piece, sent.at[stage]).wait()
    for stage, ref in ((1, buf_b), (2, got_b.at[:, :, :, :, :, real]), (3, got_c.at[:, :, :, :, :, real]), (4, got_c.at[:, :, :, :, :, real]), (5, got_e.at[:, :, :, :, :, real]), (6, buf_b)):
        pltpu.make_async_copy(ref, ref, sent.at[stage]).wait()


def shards(thermal_field, seasonal_bucket, season_of_record):
    days_here, cells = thermal_field.shape
    blocks = cells // 128
    x = thermal_field.reshape(days_here, blocks, 128).transpose(1, 0, 2)
    x = x.reshape(blocks // 2, 2 * days_here, 128)
    tiles = blocks // 2 // 3
    na, nv = tiles // Q // 8, tiles // Q // 64
    hbm = pl.BlockSpec(memory_space=pl.ANY)
    out = pl.pallas_call(
        kernel,
        out_shape=pltpu.VMEM(x.shape, F32),
        in_specs=[hbm] * 5,
        out_specs=hbm,
        scratch_shapes=[
            pltpu.VMEM((3, Q, 8, na, 8, 128), F32),
            pltpu.VMEM((3, Q, 2, 8, na // 4, 8, 128), F32),
            pltpu.VMEM((3, Q, 2, 4, nv, PART, 128), F32),
            pltpu.VMEM((3, Q, 4, 2, nv, PART, 128), F32),
            pltpu.VMEM((3, Q, 2, 4, nv, PART, 128), F32),
            pltpu.VMEM((3, Q, 3, 2, nv, PART, 128), F32),
            pltpu.VMEM((3, Q, 4, 2, nv, PART, 128), F32),
            pltpu.VMEM((3, Q, 2, 4, nv, PART, 128), F32),
            pltpu.VMEM((3, Q, 2, 8, na // 4, 8, 128), F32),
            pltpu.VMEM((3, Q, 8, na, 8, 128), F32),
            pltpu.VMEM((3, 2, 128, 256), BF16),
            pltpu.VMEM((3, 2, ROWS, 256), BF16),
            pltpu.VMEM((4, PART, 128), F32),
            pltpu.VMEM((4, 128), jnp.int32),
            pltpu.VMEM((4, 128), jnp.int32),
            pltpu.SMEM((512,), jnp.int32),
            pltpu.SMEM((512,), jnp.int32),
            pltpu.SemaphoreType.DMA((8, 3, Q, 2)),
            pltpu.SemaphoreType.DMA((8,)),
            pltpu.SemaphoreType.DMA((4,)),
        ],
        compiler_params=pltpu.CompilerParams(
            collective_id=0, has_side_effects=True, vmem_limit_bytes=63_880_000
        ),
    )(
        x,
        seasonal_bucket.reshape(4, 128),
        season_of_record.reshape(4, 128),
        seasonal_bucket,
        season_of_record,
    )
    out = out.reshape(blocks, days_here, 128).transpose(1, 0, 2)
    return out.reshape(days_here, cells)


def solution(mesh):
    placed = (P(("tm", "space"), None), P(), P())
    return jax.shard_map(
        shards, mesh=mesh, in_specs=placed, out_specs=P(("tm", "space"), None), check_vma=False
    )
```

```python
import functools

import jax
import jax.numpy as jnp
from jax import lax
from jax.experimental import pallas as pl
from jax.experimental.pallas import tpu as pltpu
from jax.sharding import PartitionSpec as P

GROUPS = 46
BASE_YEARS = 6
MIDDLE = 250.0
MESH = pl.DeviceIdType.MESH
F32, BF16 = jnp.float32, jnp.bfloat16

TOGETHER = (0, 1, 2, 3, 4, 5, 6, 7)
Q = 4
HALF = 48
ROWS = 2 * HALF
PART = ROWS // 4
REAL = GROUPS // 2


def coordinates():
    tm, space = lax.axis_index("tm"), lax.axis_index("space")
    x = lax.rem(lax.div(space, 2), 2) * 2 + lax.div(tm, 4)
    return (x, lax.rem(tm, 4), lax.div(space, 4), lax.rem(space, 2))


def device(x, y, z, core):
    return (lax.rem(x, 2) * 4 + y, z * 4 + lax.div(x, 2) * 2 + core)


def peer(me, axis, step, core_step=0):
    at = list(me)
    at[axis] = lax.rem(me[axis] + step, 4)
    at[3] = lax.rem(me[3] + core_step, 2)
    return at


def dot2(one_hot_twice, v):
    high = v.astype(BF16)
    low = (v - high.astype(F32)).astype(BF16)
    return jnp.dot(one_hot_twice, jnp.concatenate([high, low], axis=0), preferred_element_type=F32)


def halving(at, axis, h):
    m = at[axis]
    up = lax.rem(m + h, 2) == 0
    one, two = jnp.where(up, 1, 3), jnp.where(up, 3, 1)
    u = lax.rem(lax.div(m + 1 - h, 2), 2)
    v = lax.rem(m, 2) if h else lax.div(m, 2)
    return peer(at, axis, one), peer(at, axis, two), u, v


def kernel(
    x_ref, bucket_rows, year_rows, bucket_hbm, year_hbm, out_ref,
    buf_a, buf_b, part, kept, got_b, got_c, mean, got_e, buf_y, buf_z,
    member, base_t, counts, bucket_row, year_row, bucket, year, recv, sent, small,
):
    me = coordinates()
    tiles = x_ref.shape[0] // 3
    chunk = tiles // Q
    na = chunk // 8
    nh, nu, nv = na // 2, na // 4, na // 8
    real = pl.ds(0, REAL)

    loads = [
        pltpu.make_async_copy(src, dst, small.at[i])
        for i, (src, dst) in enumerate(
            ((bucket_hbm, bucket), (year_hbm, year), (bucket_rows, bucket_row), (year_rows, year_row))
        )
    ]
    for load in loads:
        load.start()

    barrier = pltpu.get_barrier_semaphore()
    partners = 0
    for axis in range(3):
        for step in range(1, 4):
            for core in range(2):
                pl.semaphore_signal(barrier, inc=1, device_id=device(*peer(me, axis, step, core)), device_id_type=MESH)
                partners += 1
    pl.semaphore_signal(barrier, inc=1, device_id=device(*peer(me, 0, 0, 1)), device_id_type=MESH)
    pl.semaphore_wait(barrier, partners + 1)

    def slot(stage, t, q):
        at = sum(Q if k in TOGETHER else 3 * Q for k in range(stage))
        return recv.at[at + q if stage in TOGETHER else at + 3 * q + t]

    def remote(src, dst, stage, t, q, to):
        pltpu.make_async_remote_copy(
            src_ref=src, dst_ref=dst, send_sem=sent.at[stage], recv_sem=slot(stage, t, q),
            device_id=device(*to), device_id_type=MESH,
        ).start()

    def local(src, dst, stage, t, q):
        pltpu.make_async_copy(src, dst, slot(stage, t, q)).start()

    def arrive(stage, t, q):
        if stage in TOGETHER and t > 0:
            return
        thirds = slice(None) if stage in TOGETHER else t
        ref = (
            buf_a.at[thirds, q], buf_b.at[thirds, q], got_b.at[thirds, q, :, :, :, real],
            got_c.at[thirds, q, :, :, :, real], mean.at[thirds, q, pl.ds(0, 3), :, :, real],
            got_e.at[thirds, q, :, :, :, real], buf_y.at[thirds, q], buf_z.at[thirds, q],
        )[stage]
        pltpu.make_async_copy(ref, ref, slot(stage, t, q)).wait()

    def axes(t):
        return t, (t + 1) % 3, (t + 2) % 3

    order = ((1, 0), (3, 0), (2, 0), (1, 1), (3, 1), (2, 1), (0, 1))
    row = lax.broadcasted_iota(jnp.int32, (4, PART, 128), 1)
    pairs = [(t, h) for t in range(3) for h in range(2)]

    def send_a(q):
        for t in range(3):
            mine = me[t] * 2 + me[3]
            local(x_ref.at[pl.ds(t * tiles + q * chunk + mine * na, na)], buf_a.at[t, q, mine], 0, t, q)
        for step, core in order:
            for t in range(3):
                to = peer(me, t, step, core)
                mine, theirs = me[t] * 2 + me[3], to[t] * 2 + to[3]
                remote(x_ref.at[pl.ds(t * tiles + q * chunk + theirs * na, na)], buf_a.at[t, q, mine], 0, t, q, to)

    def send_b1(q):
        for t, h in pairs:
            if h == 0:
                arrive(0, t, q)
            one, _, u, _ = halving(me, axes(t)[1], h)
            remote(buf_a.at[t, q, :, pl.ds(h * nh + (1 - u) * nu, nu)], buf_b.at[t, q, h], 1, t, q, one)

    def send_b2(q):
        for t in range(3):
            sums = []
            for h in range(2):
                _, _, u, v = halving(me, axes(t)[1], h)
                if h == 0:
                    arrive(1, t, q)
                columns = []
                for half in (1 - v, v):
                    for n in range(nv):
                        k = half * nv + n
                        mine = buf_a[t, q, :, h * nh + u * nu + k].reshape(64, 128)
                        theirs = buf_b[t, q, h, :, k].reshape(64, 128)
                        columns.append(jnp.concatenate([mine, theirs], axis=0))
                sums.append(dot2(base_t[t, h], jnp.concatenate(columns, axis=1) - MIDDLE))
            for h in range(2):
                for n in range(nv):
                    for j in range(4):
                        rows = slice(PART * j, PART * (j + 1))
                        part[t, q, h, j, n] = sums[h][rows, 128 * n : 128 * (n + 1)]
                        kept[t, q, j, h, n] = sums[h][rows, 128 * (nv + n) : 128 * (nv + n + 1)]
            for h in range(2):
                two = halving(me, axes(t)[1], h)[1]
                remote(part.at[t, q, h, :, :, real], got_b.at[t, q, h, :, :, real], 2, t, q, two)

    def send_c(q):
        for t in range(3):
            c = axes(t)[2]
            arrive(2, t, q)
            for h in range(2):
                for j in range(4):
                    kept[t, q, j, h] += got_b[t, q, h, j]
            for step in (1, 3, 2):
                to = peer(me, c, step)
                remote(kept.at[t, q, to[c], :, :, real], got_c.at[t, q, step - 1, :, :, real], 3, t, q, to)

    def send_d(q):
        for t in range(3):
            c = axes(t)[2]
            arrive(3, t, q)
            total = (kept[t, q, me[c]] + got_c[t, q, 0]) + (got_c[t, q, 1] + got_c[t, q, 2])
            mean[t, q, me[c]] = total / counts[me[c]][None, None]
            for step in (1, 3, 2):
                to = peer(me, c, step)
                remote(mean.at[t, q, me[c], :, :, real], mean.at[t, q, me[c], :, :, real], 4, t, q, to)

    def send_e2(q):
        for t in range(3):
            arrive(4, t, q)
            for h in range(2):
                two = halving(me, axes(t)[1], h)[1]
                remote(mean.at[t, q, :, h, :, real], got_e.at[t, q, h, :, :, real], 5, t, q, two)

    def send_e1(q):
        for t in range(3):
            chosen = []
            for h in range(2):
                if h == 0:
                    arrive(5, t, q)
                rows = jnp.concatenate(
                    [jnp.where(row < REAL, mean[t, q, :, h, n], 0.0).reshape(ROWS, 128) for n in range(nv)]
                    + [jnp.where(row < REAL, got_e[t, q, h, :, n], 0.0).reshape(ROWS, 128) for n in range(nv)],
                    axis=1,
                )
                rows = jnp.concatenate([rows, jnp.zeros((128 - ROWS, 128 * nu), F32)], axis=0)
                chosen.append(dot2(member[t, h], rows))
            for h in range(2):
                one, _, u, v = halving(me, axes(t)[1], h)
                at = h * nh + u * nu
                for k in range(nu):
                    to = (v if k < nv else 1 - v) * nv + k % nv
                    column = chosen[h][64:, 128 * k : 128 * (k + 1)]
                    buf_y[t, q, h, :, to] = (buf_b[t, q, h, :, to] - MIDDLE) - column.reshape(8, 8, 128)
                remote(buf_y.at[t, q, h], buf_z.at[t, q, :, pl.ds(at, nu)], 6, t, q, one)
            for h in range(2):
                _, _, u, v = halving(me, axes(t)[1], h)
                at = h * nh + u * nu
                for k in range(nu):
                    to = at + (v if k < nv else 1 - v) * nv + k % nv
                    column = chosen[h][:64, 128 * k : 128 * (k + 1)]
                    buf_z[t, q, :, to] = (buf_a[t, q, :, to] - MIDDLE) - column.reshape(8, 8, 128)

    def ranked(axis):
        m = me[axis]
        first = jnp.where(m == 0, 1, 0)
        second = jnp.where(m == 0, 3, jnp.where(m == 2, 1, 2))
        third = jnp.where(m == 0, 2, jnp.where(m == 3, 1, 3))
        return first, second, third

    def send_f(q, ranks):
        for t in range(3):
            mine = me[t] * 2 + me[3]
            here = out_ref.at[pl.ds(t * tiles + q * chunk + mine * na, na)]
            if 0 in ranks:
                arrive(6, t, q)
                to = peer(me, t, 0, 1)
                remote(buf_z.at[t, q, to[t] * 2 + to[3]], here, 7, t, q, to)
                local(buf_z.at[t, q, mine], here, 7, t, q)
            for rank in ranks:
                for core in (1, 0):
                    to = list(me)
                    to[t], to[3] = ranked(t)[rank], core
                    remote(buf_z.at[t, q, to[t] * 2 + core], here, 7, t, q, to)

    def finish(q):
        for t in range(3):
            arrive(7, t, q)

    def place(group):
        return group + jnp.where(group < REAL, 0, 1)

    def prepare():
        for load in loads:
            load.wait()
        group = lax.broadcasted_iota(jnp.int32, (HALF, 128), 0)
        seen = jnp.zeros((HALF, 128), F32)
        for r in range(4):
            days_row = jnp.where(year_row[r : r + 1] < BASE_YEARS, place(bucket_row[r : r + 1]), -1)
            seen = seen + jnp.where(days_row == group, 1.0, 0.0)
        number = jnp.maximum(jnp.sum(seen, axis=1, keepdims=True), 1.0)
        number = jnp.broadcast_to(number, (HALF, 128))
        for j in range(4):
            at = (j % 2) * PART
            counts[j] = number[at : at + PART]
        sub = lax.broadcasted_iota(jnp.int32, (8, 128), 0)
        lane = lax.broadcasted_iota(jnp.int32, (8, 128), 1)
        day, column = lax.rem(sub, 4), lane - lax.div(sub, 4) * HALF

        def pick(v):
            chosen = jnp.where(day == 0, v[0], jnp.where(day == 1, v[1], jnp.where(day == 2, v[2], v[3])))
            return jnp.where(chosen == column, 1.0, 0.0)

        def line(at, a):
            every, based = [], []
            for i in range(8):
                who = list(at)
                who[a], who[3] = i // 2, i % 2
                tm, space = device(*who)
                first = (tm * 16 + space) * 4
                groups = [place(bucket[first + d]) for d in range(4)]
                every.append(pick(groups))
                based.append(pick([jnp.where(year[first + d] < BASE_YEARS, groups[d], -1000) for d in range(4)]))
            return every, based

        for t in range(3):
            a, b, _ = axes(t)
            mine, mine_base = line(me, a)
            for h in range(2):
                theirs, theirs_base = line(halving(me, b, h)[0], a)
                every = jnp.concatenate(mine + theirs, axis=0).astype(BF16)
                based = jnp.concatenate(mine_base + theirs_base, axis=0).T[:ROWS].astype(BF16)
                member[t, h] = jnp.concatenate([every, every], axis=1)
                base_t[t, h] = jnp.concatenate([based, based], axis=1)

    stages = (send_a, send_b1, send_b2, send_c, send_d, send_e2, send_e1, send_f)
    stages[0](0)
    stages[0](1)
    stages[0](2)
    stages[0](3)
    prepare()
    stages[1](0)
    stages[1](1)
    stages[1](2)
    stages[1](3)
    stages[2](0)
    stages[2](1)
    stages[2](2)
    stages[2](3)
    stages[3](0)
    stages[3](1)
    stages[3](2)
    stages[3](3)
    stages[4](0)
    stages[4](1)
    stages[4](2)
    stages[4](3)
    stages[5](0)
    stages[5](1)
    stages[5](2)
    stages[5](3)
    stages[6](0)
    stages[6](1)
    stages[6](2)
    stages[6](3)
    send_f(0, (0, 1, 2))
    send_f(1, (0, 1, 2))
    send_f(2, (0, 1, 2))
    send_f(3, (0, 1, 2))
    for q in range(Q):
        finish(q)

    for stage, ref in ((0, buf_a), (7, buf_z)):
        for t in range(3):
            for q in range(Q):
                piece = ref.at[t, q, pl.ds(0, 7)]
                pltpu.make_async_copy(piece, piece, sent.at[stage]).wait()
    for stage, ref in ((1, buf_b), (2, got_b.at[:, :, :, :, :, real]), (3, got_c.at[:, :, :, :, :, real]), (4, got_c.at[:, :, :, :, :, real]), (5, got_e.at[:, :, :, :, :, real]), (6, buf_b)):
        pltpu.make_async_copy(ref, ref, sent.at[stage]).wait()


def shards(thermal_field, seasonal_bucket, season_of_record):
    days_here, cells = thermal_field.shape
    blocks = cells // 128
    x = thermal_field.reshape(days_here, blocks, 128).transpose(1, 0, 2)
    x = x.reshape(blocks // 2, 2 * days_here, 128)
    tiles = blocks // 2 // 3
    na, nv = tiles // Q // 8, tiles // Q // 64
    hbm = pl.BlockSpec(memory_space=pl.ANY)
    out = pl.pallas_call(
        kernel,
        out_shape=pltpu.VMEM(x.shape, F32),
        in_specs=[hbm] * 5,
        out_specs=hbm,
        scratch_shapes=[
            pltpu.VMEM((3, Q, 8, na, 8, 128), F32),
            pltpu.VMEM((3, Q, 2, 8, na // 4, 8, 128), F32),
            pltpu.VMEM((3, Q, 2, 4, nv, PART, 128), F32),
            pltpu.VMEM((3, Q, 4, 2, nv, PART, 128), F32),
            pltpu.VMEM((3, Q, 2, 4, nv, PART, 128), F32),
            pltpu.VMEM((3, Q, 3, 2, nv, PART, 128), F32),
            pltpu.VMEM((3, Q, 4, 2, nv, PART, 128), F32),
            pltpu.VMEM((3, Q, 2, 4, nv, PART, 128), F32),
            pltpu.VMEM((3, Q, 2, 8, na // 4, 8, 128), F32),
            pltpu.VMEM((3, Q, 8, na, 8, 128), F32),
            pltpu.VMEM((3, 2, 128, 256), BF16),
            pltpu.VMEM((3, 2, ROWS, 256), BF16),
            pltpu.VMEM((4, PART, 128), F32),
            pltpu.VMEM((4, 128), jnp.int32),
            pltpu.VMEM((4, 128), jnp.int32),
            pltpu.SMEM((512,), jnp.int32),
            pltpu.SMEM((512,), jnp.int32),
            pltpu.SemaphoreType.DMA((sum(Q if k in TOGETHER else 3 * Q for k in range(8)),)),
            pltpu.SemaphoreType.DMA((8,)),
            pltpu.SemaphoreType.DMA((4,)),
        ],
        compiler_params=pltpu.CompilerParams(
            collective_id=0, has_side_effects=True, vmem_limit_bytes=63_880_000
        ),
    )(
        x,
        seasonal_bucket.reshape(4, 128),
        season_of_record.reshape(4, 128),
        seasonal_bucket,
        season_of_record,
    )
    out = out.reshape(blocks, days_here, 128).transpose(1, 0, 2)
    return out.reshape(days_here, cells)


def solution(mesh):
    placed = (P(("tm", "space"), None), P(), P())
    return jax.shard_map(
        shards, mesh=mesh, in_specs=placed, out_specs=P(("tm", "space"), None), check_vma=False
    )
```

```python
import functools

import jax
import jax.numpy as jnp
from jax import lax
from jax.experimental import pallas as pl
from jax.experimental.pallas import tpu as pltpu
from jax.sharding import PartitionSpec as P

GROUPS = 46
BASE_YEARS = 6
MIDDLE = 250.0
MESH = pl.DeviceIdType.MESH
F32, BF16 = jnp.float32, jnp.bfloat16

Q = 4
LAST = 7 * Q
HALF = 48
ROWS = 2 * HALF
PART = ROWS // 4
REAL = GROUPS // 2


def coordinates():
    tm, space = lax.axis_index("tm"), lax.axis_index("space")
    x = lax.rem(lax.div(space, 2), 2) * 2 + lax.div(tm, 4)
    return (x, lax.rem(tm, 4), lax.div(space, 4), lax.rem(space, 2))


def device(x, y, z, core):
    return (lax.rem(x, 2) * 4 + y, z * 4 + lax.div(x, 2) * 2 + core)


def peer(me, axis, step, core_step=0):
    at = list(me)
    at[axis] = lax.rem(me[axis] + step, 4)
    at[3] = lax.rem(me[3] + core_step, 2)
    return at


def dot2(one_hot_twice, v):
    high = v.astype(BF16)
    low = (v - high.astype(F32)).astype(BF16)
    return jnp.dot(one_hot_twice, jnp.concatenate([high, low], axis=0), preferred_element_type=F32)


def halving(at, axis, h):
    m = at[axis]
    up = lax.rem(m + h, 2) == 0
    one, two = jnp.where(up, 1, 3), jnp.where(up, 3, 1)
    u = lax.rem(lax.div(m + 1 - h, 2), 2)
    v = lax.rem(m, 2) if h else lax.div(m, 2)
    return peer(at, axis, one), peer(at, axis, two), u, v


def kernel(
    x_ref, bucket_rows, year_rows, bucket_hbm, year_hbm, out_ref,
    buf_a, buf_b, part, kept, got_b, got_c, mean, got_e, buf_y, buf_z,
    member, base_t, counts, bucket_row, year_row, bucket, year, recv, sent, small,
):
    me = coordinates()
    tiles = x_ref.shape[0] // 3
    chunk = tiles // Q
    na = chunk // 8
    nh, nu, nv = na // 2, na // 4, na // 8
    real = pl.ds(0, REAL)

    loads = [
        pltpu.make_async_copy(src, dst, small.at[i])
        for i, (src, dst) in enumerate(
            ((bucket_hbm, bucket), (year_hbm, year), (bucket_rows, bucket_row), (year_rows, year_row))
        )
    ]
    for load in loads:
        load.start()

    barrier = pltpu.get_barrier_semaphore()
    partners = 0
    for axis in range(3):
        for step in (2, 1, 3):
            for core in range(2):
                pl.semaphore_signal(barrier, inc=1, device_id=device(*peer(me, axis, step, core)), device_id_type=MESH)
                partners += 1
    pl.semaphore_signal(barrier, inc=1, device_id=device(*peer(me, 0, 0, 1)), device_id_type=MESH)
    pl.semaphore_wait(barrier, partners + 1)

    def remote(src, dst, stage, q, to):
        pltpu.make_async_remote_copy(
            src_ref=src, dst_ref=dst, send_sem=sent.at[stage], recv_sem=recv.at[min(Q * stage + q, LAST)],
            device_id=device(*to), device_id_type=MESH,
        ).start()

    def local(src, dst, stage, q):
        pltpu.make_async_copy(src, dst, recv.at[min(Q * stage + q, LAST)]).start()

    def arrive(stage, q):
        ref = (
            buf_a.at[:, q], buf_b.at[:, q], got_b.at[:, q, :, :, :, real],
            got_c.at[:, q, :, :, :, real], mean.at[:, q, pl.ds(0, 3), :, :, real],
            got_e.at[:, q, :, :, :, real], buf_y.at[:, q], buf_z,
        )[stage]
        pltpu.make_async_copy(ref, ref, recv.at[min(Q * stage + q, LAST)]).wait()

    def axes(t):
        return t, (t + 1) % 3, (t + 2) % 3

    order = ((2, 0), (2, 1), (1, 0), (3, 0), (1, 1), (3, 1), (0, 1))
    row = lax.broadcasted_iota(jnp.int32, (4, PART, 128), 1)
    pairs = [(t, h) for t in range(3) for h in range(2)]

    def send_a(q):
        for t in range(3):
            mine = me[t] * 2 + me[3]
            local(x_ref.at[pl.ds(t * tiles + q * chunk + mine * na, na)], buf_a.at[t, q, mine], 0, q)
        for step, core in order:
            for t in range(3):
                to = peer(me, t, step, core)
                mine, theirs = me[t] * 2 + me[3], to[t] * 2 + to[3]
                remote(x_ref.at[pl.ds(t * tiles + q * chunk + theirs * na, na)], buf_a.at[t, q, mine], 0, q, to)

    def send_b1(q):
        arrive(0, q)
        for t, h in pairs:
            one, _, u, _ = halving(me, axes(t)[1], h)
            remote(buf_a.at[t, q, :, pl.ds(h * nh + (1 - u) * nu, nu)], buf_b.at[t, q, h], 1, q, one)

    def send_b2(q):
        arrive(1, q)
        for t in range(3):
            sums = []
            for h in range(2):
                _, _, u, v = halving(me, axes(t)[1], h)
                columns = []
                for half in (1 - v, v):
                    for n in range(nv):
                        k = half * nv + n
                        mine = buf_a[t, q, :, h * nh + u * nu + k].reshape(64, 128)
                        theirs = buf_b[t, q, h, :, k].reshape(64, 128)
                        columns.append(jnp.concatenate([mine, theirs], axis=0))
                sums.append(dot2(base_t[t, h], jnp.concatenate(columns, axis=1) - MIDDLE))
            for h in range(2):
                for n in range(nv):
                    for j in range(4):
                        rows = slice(PART * j, PART * (j + 1))
                        part[t, q, h, j, n] = sums[h][rows, 128 * n : 128 * (n + 1)]
                        kept[t, q, j, h, n] = sums[h][rows, 128 * (nv + n) : 128 * (nv + n + 1)]
            for h in range(2):
                two = halving(me, axes(t)[1], h)[1]
                remote(part.at[t, q, h, :, :, real], got_b.at[t, q, h, :, :, real], 2, q, two)

    def send_c(q):
        arrive(2, q)
        for t in range(3):
            c = axes(t)[2]
            for h in range(2):
                for j in range(4):
                    kept[t, q, j, h] += got_b[t, q, h, j]
            for step in (2, 1, 3):
                to = peer(me, c, step)
                remote(kept.at[t, q, to[c], :, :, real], got_c.at[t, q, step - 1, :, :, real], 3, q, to)

    def send_d(q):
        arrive(3, q)
        for t in range(3):
            c = axes(t)[2]
            total = (kept[t, q, me[c]] + got_c[t, q, 0]) + (got_c[t, q, 1] + got_c[t, q, 2])
            mean[t, q, me[c]] = total / counts[me[c]][None, None]
            for step in (2, 1, 3):
                to = peer(me, c, step)
                remote(mean.at[t, q, me[c], :, :, real], mean.at[t, q, me[c], :, :, real], 4, q, to)

    def send_e2(q):
        arrive(4, q)
        for t in range(3):
            for h in range(2):
                two = halving(me, axes(t)[1], h)[1]
                remote(mean.at[t, q, :, h, :, real], got_e.at[t, q, h, :, :, real], 5, q, two)

    def send_e1(q):
        arrive(5, q)
        for t in range(3):
            chosen = []
            for h in range(2):
                rows = jnp.concatenate(
                    [jnp.where(row < REAL, mean[t, q, :, h, n], 0.0).reshape(ROWS, 128) for n in range(nv)]
                    + [jnp.where(row < REAL, got_e[t, q, h, :, n], 0.0).reshape(ROWS, 128) for n in range(nv)],
                    axis=1,
                )
                rows = jnp.concatenate([rows, jnp.zeros((128 - ROWS, 128 * nu), F32)], axis=0)
                chosen.append(dot2(member[t, h], rows))
            for h in range(2):
                one, _, u, v = halving(me, axes(t)[1], h)
                at = h * nh + u * nu
                for k in range(nu):
                    to = (v if k < nv else 1 - v) * nv + k % nv
                    column = chosen[h][64:, 128 * k : 128 * (k + 1)]
                    buf_y[t, q, h, :, to] = (buf_b[t, q, h, :, to] - MIDDLE) - column.reshape(8, 8, 128)
                remote(buf_y.at[t, q, h], buf_z.at[t, q, :, pl.ds(at, nu)], 6, q, one)
            for h in range(2):
                _, _, u, v = halving(me, axes(t)[1], h)
                at = h * nh + u * nu
                for k in range(nu):
                    to = at + (v if k < nv else 1 - v) * nv + k % nv
                    column = chosen[h][:64, 128 * k : 128 * (k + 1)]
                    buf_z[t, q, :, to] = (buf_a[t, q, :, to] - MIDDLE) - column.reshape(8, 8, 128)

    def send_f(q):
        arrive(6, q)
        for t in range(3):
            mine = me[t] * 2 + me[3]
            here = out_ref.at[pl.ds(t * tiles + q * chunk + mine * na, na)]
            for step, core in order:
                to = peer(me, t, step, core)
                remote(buf_z.at[t, q, to[t] * 2 + to[3]], here, 7, q, to)
            local(buf_z.at[t, q, mine], here, 7, q)

    def place(group):
        return group + jnp.where(group < REAL, 0, 1)

    def prepare():
        for load in loads:
            load.wait()
        group = lax.broadcasted_iota(jnp.int32, (HALF, 128), 0)
        seen = jnp.zeros((HALF, 128), F32)
        for r in range(4):
            days_row = jnp.where(year_row[r : r + 1] < BASE_YEARS, place(bucket_row[r : r + 1]), -1)
            seen = seen + jnp.where(days_row == group, 1.0, 0.0)
        number = jnp.maximum(jnp.sum(seen, axis=1, keepdims=True), 1.0)
        number = jnp.broadcast_to(number, (HALF, 128))
        for j in range(4):
            at = (j % 2) * PART
            counts[j] = number[at : at + PART]
        sub = lax.broadcasted_iota(jnp.int32, (8, 128), 0)
        lane = lax.broadcasted_iota(jnp.int32, (8, 128), 1)
        day, column = lax.rem(sub, 4), lane - lax.div(sub, 4) * HALF

        def pick(v):
            chosen = jnp.where(day == 0, v[0], jnp.where(day == 1, v[1], jnp.where(day == 2, v[2], v[3])))
            return jnp.where(chosen == column, 1.0, 0.0)

        def line(at, a):
            every, based = [], []
            for i in range(8):
                who = list(at)
                who[a], who[3] = i // 2, i % 2
                tm, space = device(*who)
                first = (tm * 16 + space) * 4
                groups = [place(bucket[first + d]) for d in range(4)]
                every.append(pick(groups))
                based.append(pick([jnp.where(year[first + d] < BASE_YEARS, groups[d], -1000) for d in range(4)]))
            return every, based

        for t in range(3):
            a, b, _ = axes(t)
            mine, mine_base = line(me, a)
            for h in range(2):
                theirs, theirs_base = line(halving(me, b, h)[0], a)
                every = jnp.concatenate(mine + theirs, axis=0).astype(BF16)
                based = jnp.concatenate(mine_base + theirs_base, axis=0).T[:ROWS].astype(BF16)
                member[t, h] = jnp.concatenate([every, every], axis=1)
                base_t[t, h] = jnp.concatenate([based, based], axis=1)

    stages = (send_a, send_b1, send_b2, send_c, send_d, send_e2, send_e1, send_f)
    stages[0](0)
    stages[0](1)
    stages[0](2)
    prepare()
    stages[1](0)
    stages[0](3)
    stages[1](1)
    stages[1](2)
    stages[1](3)
    stages[2](0)
    stages[2](1)
    stages[2](2)
    stages[2](3)
    stages[3](0)
    stages[3](1)
    stages[3](2)
    stages[3](3)
    stages[4](0)
    stages[4](1)
    stages[4](2)
    stages[4](3)
    stages[5](0)
    stages[5](1)
    stages[5](2)
    stages[5](3)
    stages[6](0)
    stages[6](1)
    stages[6](2)
    stages[6](3)
    stages[7](0)
    stages[7](1)
    stages[7](2)
    stages[7](3)
    arrive(7, 0)

    for stage, ref in (
        (0, buf_a.at[:, :, pl.ds(0, 7)]), (1, buf_b), (2, got_b.at[:, :, :, :, :, real]), (3, got_c.at[:, :, :, :, :, real]),
        (4, got_c.at[:, :, :, :, :, real]), (5, got_e.at[:, :, :, :, :, real]), (6, buf_b), (7, buf_z.at[:, :, pl.ds(0, 7)]),
    ):
        pltpu.make_async_copy(ref, ref, sent.at[stage]).wait()


def shards(thermal_field, seasonal_bucket, season_of_record):
    days_here, cells = thermal_field.shape
    blocks = cells // 128
    x = thermal_field.reshape(days_here, blocks, 128).transpose(1, 0, 2)
    x = x.reshape(blocks // 2, 2 * days_here, 128)
    tiles = blocks // 2 // 3
    na, nv = tiles // Q // 8, tiles // Q // 64
    hbm = pl.BlockSpec(memory_space=pl.ANY)
    out = pl.pallas_call(
        kernel,
        out_shape=pltpu.VMEM(x.shape, F32),
        in_specs=[hbm] * 5,
        out_specs=hbm,
        scratch_shapes=[
            pltpu.VMEM((3, Q, 8, na, 8, 128), F32),
            pltpu.VMEM((3, Q, 2, 8, na // 4, 8, 128), F32),
            pltpu.VMEM((3, Q, 2, 4, nv, PART, 128), F32),
            pltpu.VMEM((3, Q, 4, 2, nv, PART, 128), F32),
            pltpu.VMEM((3, Q, 2, 4, nv, PART, 128), F32),
            pltpu.VMEM((3, Q, 3, 2, nv, PART, 128), F32),
            pltpu.VMEM((3, Q, 4, 2, nv, PART, 128), F32),
            pltpu.VMEM((3, Q, 2, 4, nv, PART, 128), F32),
            pltpu.VMEM((3, Q, 2, 8, na // 4, 8, 128), F32),
            pltpu.VMEM((3, Q, 8, na, 8, 128), F32),
            pltpu.VMEM((3, 2, 128, 256), BF16),
            pltpu.VMEM((3, 2, ROWS, 256), BF16),
            pltpu.VMEM((4, PART, 128), F32),
            pltpu.VMEM((4, 128), jnp.int32),
            pltpu.VMEM((4, 128), jnp.int32),
            pltpu.SMEM((512,), jnp.int32),
            pltpu.SMEM((512,), jnp.int32),
            pltpu.SemaphoreType.DMA((LAST + 1,)),
            pltpu.SemaphoreType.DMA((8,)),
            pltpu.SemaphoreType.DMA((4,)),
        ],
        compiler_params=pltpu.CompilerParams(
            collective_id=0, has_side_effects=True, vmem_limit_bytes=63_880_000
        ),
    )(
        x,
        seasonal_bucket.reshape(4, 128),
        season_of_record.reshape(4, 128),
        seasonal_bucket,
        season_of_record,
    )
    out = out.reshape(blocks, days_here, 128).transpose(1, 0, 2)
    return out.reshape(days_here, cells)


def solution(mesh):
    placed = (P(("tm", "space"), None), P(), P())
    return jax.shard_map(
        shards, mesh=mesh, in_specs=placed, out_specs=P(("tm", "space"), None), check_vma=False
    )
```

```python
import functools

import jax
import jax.numpy as jnp
from jax import lax
from jax.experimental import pallas as pl
from jax.experimental.pallas import tpu as pltpu
from jax.sharding import PartitionSpec as P

GROUPS = 46
BASE_YEARS = 6
MIDDLE = 250.0
MESH = pl.DeviceIdType.MESH
F32, BF16 = jnp.float32, jnp.bfloat16

Q = 4
LAST = 7 * Q
HALF = 48
ROWS = 2 * HALF
PART = ROWS // 4
REAL = GROUPS // 2


def coordinates():
    tm, space = lax.axis_index("tm"), lax.axis_index("space")
    x = lax.rem(lax.div(space, 2), 2) * 2 + lax.div(tm, 4)
    return (x, lax.rem(tm, 4), lax.div(space, 4), lax.rem(space, 2))


def device(x, y, z, core):
    return (lax.rem(x, 2) * 4 + y, z * 4 + lax.div(x, 2) * 2 + core)


def peer(me, axis, step, core_step=0):
    at = list(me)
    at[axis] = lax.rem(me[axis] + step, 4)
    at[3] = lax.rem(me[3] + core_step, 2)
    return at


def dot3(one_hot_thrice, v):
    high = v.astype(BF16)
    rest = v - high.astype(F32)
    middle = rest.astype(BF16)
    low = (rest - middle.astype(F32)).astype(BF16)
    return jnp.dot(one_hot_thrice, jnp.concatenate([high, middle, low], axis=0), preferred_element_type=F32)


def halving(at, axis, h):
    m = at[axis]
    up = lax.rem(m + h, 2) == 0
    one, two = jnp.where(up, 1, 3), jnp.where(up, 3, 1)
    u = lax.rem(lax.div(m + 1 - h, 2), 2)
    v = lax.rem(m, 2) if h else lax.div(m, 2)
    return peer(at, axis, one), peer(at, axis, two), u, v


def kernel(
    x_ref, bucket_rows, year_rows, bucket_hbm, year_hbm, out_ref,
    buf_a, buf_b, part, kept, got_b, got_c, mean, got_e, buf_y, buf_z,
    member, base_t, counts, bucket_row, year_row, bucket, year, recv, sent, small,
):
    me = coordinates()
    tiles = x_ref.shape[0] // 3
    chunk = tiles // Q
    na = chunk // 8
    nh, nu, nv = na // 2, na // 4, na // 8
    real = pl.ds(0, REAL)

    loads = [
        pltpu.make_async_copy(src, dst, small.at[i])
        for i, (src, dst) in enumerate(
            ((bucket_hbm, bucket), (year_hbm, year), (bucket_rows, bucket_row), (year_rows, year_row))
        )
    ]
    for load in loads:
        load.start()

    barrier = pltpu.get_barrier_semaphore()
    partners = 0
    for axis in range(3):
        for step in (2, 1, 3):
            for core in range(2):
                pl.semaphore_signal(barrier, inc=1, device_id=device(*peer(me, axis, step, core)), device_id_type=MESH)
                partners += 1
    pl.semaphore_signal(barrier, inc=1, device_id=device(*peer(me, 0, 0, 1)), device_id_type=MESH)
    pl.semaphore_wait(barrier, partners + 1)

    def remote(src, dst, stage, q, to):
        pltpu.make_async_remote_copy(
            src_ref=src, dst_ref=dst, send_sem=sent.at[stage], recv_sem=recv.at[min(Q * stage + q, LAST)],
            device_id=device(*to), device_id_type=MESH,
        ).start()

    def local(src, dst, stage, q):
        pltpu.make_async_copy(src, dst, recv.at[min(Q * stage + q, LAST)]).start()

    def arrive(stage, q):
        ref = (
            buf_a.at[:, q], buf_b.at[:, q], got_b.at[:, q, :, :, :, real],
            got_c.at[:, q, :, :, :, real], mean.at[:, q, pl.ds(0, 3), :, :, real],
            got_e.at[:, q, :, :, :, real], buf_y.at[:, q], buf_z,
        )[stage]
        pltpu.make_async_copy(ref, ref, recv.at[min(Q * stage + q, LAST)]).wait()

    def axes(t):
        return t, (t + 1) % 3, (t + 2) % 3

    order = ((2, 0), (2, 1), (1, 0), (3, 0), (1, 1), (3, 1), (0, 1))
    row = lax.broadcasted_iota(jnp.int32, (4, PART, 128), 1)
    pairs = [(t, h) for t in range(3) for h in range(2)]

    def send_a(q):
        for t in range(3):
            mine = me[t] * 2 + me[3]
            local(x_ref.at[pl.ds(t * tiles + q * chunk + mine * na, na)], buf_a.at[t, q, mine], 0, q)
        for step, core in order:
            for t in range(3):
                to = peer(me, t, step, core)
                mine, theirs = me[t] * 2 + me[3], to[t] * 2 + to[3]
                remote(x_ref.at[pl.ds(t * tiles + q * chunk + theirs * na, na)], buf_a.at[t, q, mine], 0, q, to)

    def send_b1(q):
        arrive(0, q)
        for t, h in pairs:
            one, _, u, _ = halving(me, axes(t)[1], h)
            remote(buf_a.at[t, q, :, pl.ds(h * nh + (1 - u) * nu, nu)], buf_b.at[t, q, h], 1, q, one)

    def send_b2(q):
        arrive(1, q)
        for t in range(3):
            sums = []
            for h in range(2):
                _, _, u, v = halving(me, axes(t)[1], h)
                columns = []
                for half in (1 - v, v):
                    for n in range(nv):
                        k = half * nv + n
                        mine = buf_a[t, q, :, h * nh + u * nu + k].reshape(64, 128)
                        theirs = buf_b[t, q, h, :, k].reshape(64, 128)
                        columns.append(jnp.concatenate([mine, theirs], axis=0))
                sums.append(dot3(base_t[t, h], jnp.concatenate(columns, axis=1) - MIDDLE))
            for h in range(2):
                for n in range(nv):
                    for j in range(4):
                        rows = slice(PART * j, PART * (j + 1))
                        part[t, q, h, j, n] = sums[h][rows, 128 * n : 128 * (n + 1)]
                        kept[t, q, j, h, n] = sums[h][rows, 128 * (nv + n) : 128 * (nv + n + 1)]
        for t, h in pairs:
            two = halving(me, axes(t)[1], h)[1]
            remote(part.at[t, q, h, :, :, real], got_b.at[t, q, h, :, :, real], 2, q, two)

    def send_c(q):
        arrive(2, q)
        for t in range(3):
            for h in range(2):
                for j in range(4):
                    kept[t, q, j, h] += got_b[t, q, h, j]
        for t in range(3):
            c = axes(t)[2]
            for step in (2, 1, 3):
                to = peer(me, c, step)
                remote(kept.at[t, q, to[c], :, :, real], got_c.at[t, q, step - 1, :, :, real], 3, q, to)

    def send_d(q):
        arrive(3, q)
        for t in range(3):
            c = axes(t)[2]
            total = (kept[t, q, me[c]] + got_c[t, q, 0]) + (got_c[t, q, 1] + got_c[t, q, 2])
            mean[t, q, me[c]] = total / counts[me[c]][None, None]
        for t in range(3):
            c = axes(t)[2]
            for step in (2, 1, 3):
                to = peer(me, c, step)
                remote(mean.at[t, q, me[c], :, :, real], mean.at[t, q, me[c], :, :, real], 4, q, to)

    def send_e2(q):
        arrive(4, q)
        for t in range(3):
            for h in range(2):
                two = halving(me, axes(t)[1], h)[1]
                remote(mean.at[t, q, :, h, :, real], got_e.at[t, q, h, :, :, real], 5, q, two)

    def send_e1(q):
        arrive(5, q)
        for t in range(3):
            chosen = []
            for h in range(2):
                rows = jnp.concatenate(
                    [jnp.where(row < REAL, mean[t, q, :, h, n], 0.0).reshape(ROWS, 128) for n in range(nv)]
                    + [jnp.where(row < REAL, got_e[t, q, h, :, n], 0.0).reshape(ROWS, 128) for n in range(nv)],
                    axis=1,
                )
                rows = jnp.concatenate([rows, jnp.zeros((128 - ROWS, 128 * nu), F32)], axis=0)
                chosen.append(dot3(member[t, h], rows))
            for h in range(2):
                v = halving(me, axes(t)[1], h)[3]
                for k in range(nu):
                    to = (v if k < nv else 1 - v) * nv + k % nv
                    column = chosen[h][64:, 128 * k : 128 * (k + 1)]
                    buf_y[t, q, h, :, to] = (buf_b[t, q, h, :, to] - MIDDLE) - column.reshape(8, 8, 128)
            for h in range(2):
                _, _, u, v = halving(me, axes(t)[1], h)
                at = h * nh + u * nu
                for k in range(nu):
                    to = at + (v if k < nv else 1 - v) * nv + k % nv
                    column = chosen[h][:64, 128 * k : 128 * (k + 1)]
                    buf_z[t, q, :, to] = (buf_a[t, q, :, to] - MIDDLE) - column.reshape(8, 8, 128)
        for t, h in pairs:
            one, _, u, _ = halving(me, axes(t)[1], h)
            remote(buf_y.at[t, q, h], buf_z.at[t, q, :, pl.ds(h * nh + u * nu, nu)], 6, q, one)

    def send_f(q):
        arrive(6, q)
        for t in range(3):
            mine = me[t] * 2 + me[3]
            here = out_ref.at[pl.ds(t * tiles + q * chunk + mine * na, na)]
            for step, core in order:
                to = peer(me, t, step, core)
                remote(buf_z.at[t, q, to[t] * 2 + to[3]], here, 7, q, to)
            local(buf_z.at[t, q, mine], here, 7, q)

    def place(group):
        return group + jnp.where(group < REAL, 0, 1)

    def prepare():
        for load in loads:
            load.wait()
        group = lax.broadcasted_iota(jnp.int32, (HALF, 128), 0)
        seen = jnp.zeros((HALF, 128), F32)
        for r in range(4):
            days_row = jnp.where(year_row[r : r + 1] < BASE_YEARS, place(bucket_row[r : r + 1]), -1)
            seen = seen + jnp.where(days_row == group, 1.0, 0.0)
        number = jnp.maximum(jnp.sum(seen, axis=1, keepdims=True), 1.0)
        number = jnp.broadcast_to(number, (HALF, 128))
        for j in range(4):
            at = (j % 2) * PART
            counts[j] = number[at : at + PART]
        sub = lax.broadcasted_iota(jnp.int32, (8, 128), 0)
        lane = lax.broadcasted_iota(jnp.int32, (8, 128), 1)
        day, column = lax.rem(sub, 4), lane - lax.div(sub, 4) * HALF

        def pick(v):
            chosen = jnp.where(day == 0, v[0], jnp.where(day == 1, v[1], jnp.where(day == 2, v[2], v[3])))
            return jnp.where(chosen == column, 1.0, 0.0)

        def line(at, a):
            every, based = [], []
            for i in range(8):
                who = list(at)
                who[a], who[3] = i // 2, i % 2
                tm, space = device(*who)
                first = (tm * 16 + space) * 4
                groups = [place(bucket[first + d]) for d in range(4)]
                every.append(pick(groups))
                based.append(pick([jnp.where(year[first + d] < BASE_YEARS, groups[d], -1000) for d in range(4)]))
            return every, based

        for t in range(3):
            a, b, _ = axes(t)
            mine, mine_base = line(me, a)
            for h in range(2):
                theirs, theirs_base = line(halving(me, b, h)[0], a)
                every = jnp.concatenate(mine + theirs, axis=0).astype(BF16)
                based = jnp.concatenate(mine_base + theirs_base, axis=0).T[:ROWS].astype(BF16)
                member[t, h] = jnp.concatenate([every] * 3, axis=1)
                base_t[t, h] = jnp.concatenate([based] * 3, axis=1)

    stages = (send_a, send_b1, send_b2, send_c, send_d, send_e2, send_e1, send_f)
    stages[0](0)
    stages[0](1)
    stages[0](2)
    prepare()
    stages[1](0)
    stages[0](3)
    stages[1](1)
    stages[1](2)
    stages[1](3)
    stages[2](0)
    stages[2](1)
    stages[2](2)
    stages[2](3)
    stages[3](0)
    stages[3](1)
    stages[3](2)
    stages[3](3)
    stages[4](0)
    stages[4](1)
    stages[4](2)
    stages[4](3)
    stages[5](0)
    stages[5](1)
    stages[5](2)
    stages[5](3)
    stages[6](0)
    stages[6](1)
    stages[6](2)
    stages[6](3)
    stages[7](0)
    stages[7](1)
    stages[7](2)
    stages[7](3)
    arrive(7, 0)

    for stage, ref in (
        (0, buf_a.at[:, :, pl.ds(0, 7)]), (1, buf_b), (2, got_b.at[:, :, :, :, :, real]), (3, got_c.at[:, :, :, :, :, real]),
        (4, got_c.at[:, :, :, :, :, real]), (5, got_e.at[:, :, :, :, :, real]), (6, buf_b), (7, buf_z.at[:, :, pl.ds(0, 7)]),
    ):
        pltpu.make_async_copy(ref, ref, sent.at[stage]).wait()


def shards(thermal_field, seasonal_bucket, season_of_record):
    days_here, cells = thermal_field.shape
    blocks = cells // 128
    x = thermal_field.reshape(days_here, blocks, 128).transpose(1, 0, 2)
    x = x.reshape(blocks // 2, 2 * days_here, 128)
    tiles = blocks // 2 // 3
    na, nv = tiles // Q // 8, tiles // Q // 64
    hbm = pl.BlockSpec(memory_space=pl.ANY)
    out = pl.pallas_call(
        kernel,
        out_shape=pltpu.VMEM(x.shape, F32),
        in_specs=[hbm] * 5,
        out_specs=hbm,
        scratch_shapes=[
            pltpu.VMEM((3, Q, 8, na, 8, 128), F32),
            pltpu.VMEM((3, Q, 2, 8, na // 4, 8, 128), F32),
            pltpu.VMEM((3, Q, 2, 4, nv, PART, 128), F32),
            pltpu.VMEM((3, Q, 4, 2, nv, PART, 128), F32),
            pltpu.VMEM((3, Q, 2, 4, nv, PART, 128), F32),
            pltpu.VMEM((3, Q, 3, 2, nv, PART, 128), F32),
            pltpu.VMEM((3, Q, 4, 2, nv, PART, 128), F32),
            pltpu.VMEM((3, Q, 2, 4, nv, PART, 128), F32),
            pltpu.VMEM((3, Q, 2, 8, na // 4, 8, 128), F32),
            pltpu.VMEM((3, Q, 8, na, 8, 128), F32),
            pltpu.VMEM((3, 2, 128, 384), BF16),
            pltpu.VMEM((3, 2, ROWS, 384), BF16),
            pltpu.VMEM((4, PART, 128), F32),
            pltpu.VMEM((4, 128), jnp.int32),
            pltpu.VMEM((4, 128), jnp.int32),
            pltpu.SMEM((512,), jnp.int32),
            pltpu.SMEM((512,), jnp.int32),
            pltpu.SemaphoreType.DMA((LAST + 1,)),
            pltpu.SemaphoreType.DMA((8,)),
            pltpu.SemaphoreType.DMA((4,)),
        ],
        compiler_params=pltpu.CompilerParams(
            collective_id=0, has_side_effects=True, vmem_limit_bytes=63_880_000
        ),
    )(
        x,
        seasonal_bucket.reshape(4, 128),
        season_of_record.reshape(4, 128),
        seasonal_bucket,
        season_of_record,
    )
    out = out.reshape(blocks, days_here, 128).transpose(1, 0, 2)
    return out.reshape(days_here, cells)


def solution(mesh):
    placed = (P(("tm", "space"), None), P(), P())
    return jax.shard_map(
        shards, mesh=mesh, in_specs=placed, out_specs=P(("tm", "space"), None), check_vma=False
    )
```

```python
import functools

import jax
import jax.numpy as jnp
from jax import lax
from jax.experimental import pallas as pl
from jax.experimental.pallas import tpu as pltpu
from jax.sharding import PartitionSpec as P

GROUPS = 46
BASE_YEARS = 6
MIDDLE = 250.0
MESH = pl.DeviceIdType.MESH
F32, BF16 = jnp.float32, jnp.bfloat16

Q = 4
LAST = 7 * Q
HALF = 48
ROWS = 2 * HALF
PART = ROWS // 4
REAL = GROUPS // 2


def coordinates():
    tm, space = lax.axis_index("tm"), lax.axis_index("space")
    x = lax.rem(lax.div(space, 2), 2) * 2 + lax.div(tm, 4)
    return (x, lax.rem(tm, 4), lax.div(space, 4), lax.rem(space, 2))


def device(x, y, z, core):
    return (lax.rem(x, 2) * 4 + y, z * 4 + lax.div(x, 2) * 2 + core)


def peer(me, axis, step, core_step=0):
    at = list(me)
    at[axis] = lax.rem(me[axis] + step, 4)
    at[3] = lax.rem(me[3] + core_step, 2)
    return at


def dot3(one_hot_thrice, v):
    high = v.astype(BF16)
    rest = v - high.astype(F32)
    middle = rest.astype(BF16)
    low = (rest - middle.astype(F32)).astype(BF16)
    return jnp.dot(one_hot_thrice, jnp.concatenate([high, middle, low], axis=0), preferred_element_type=F32)


def halving(at, axis, h):
    m = at[axis]
    up = lax.rem(m + h, 2) == 0
    one, two = jnp.where(up, 1, 3), jnp.where(up, 3, 1)
    u = lax.rem(lax.div(m + 1 - h, 2), 2)
    v = lax.rem(m, 2) if h else lax.div(m, 2)
    return peer(at, axis, one), peer(at, axis, two), u, v


def kernel(
    x_ref, bucket_rows, year_rows, bucket_hbm, year_hbm, out_ref,
    buf_a, buf_b, part, kept, got_b, got_c, mean, got_e, buf_y, buf_z,
    member, base_t, counts, bucket_row, year_row, bucket, year, recv, sent, small,
):
    me = coordinates()
    tiles = x_ref.shape[0] // 3
    chunk = tiles // Q
    na = chunk // 8
    nh, nu, nv = na // 2, na // 4, na // 8
    real = pl.ds(0, REAL)

    loads = [
        pltpu.make_async_copy(src, dst, small.at[i])
        for i, (src, dst) in enumerate(
            ((bucket_hbm, bucket), (year_hbm, year), (bucket_rows, bucket_row), (year_rows, year_row))
        )
    ]
    for load in loads:
        load.start()

    barrier = pltpu.get_barrier_semaphore()
    partners = 0
    for axis in range(3):
        for step in (2, 1, 3):
            for core in range(2):
                pl.semaphore_signal(barrier, inc=1, device_id=device(*peer(me, axis, step, core)), device_id_type=MESH)
                partners += 1
    pl.semaphore_signal(barrier, inc=1, device_id=device(*peer(me, 0, 0, 1)), device_id_type=MESH)
    pl.semaphore_wait(barrier, partners + 1)

    def remote(src, dst, stage, q, to):
        pltpu.make_async_remote_copy(
            src_ref=src, dst_ref=dst, send_sem=sent.at[0], recv_sem=recv.at[min(Q * stage + q, LAST)],
            device_id=device(*to), device_id_type=MESH,
        ).start()

    def local(src, dst, stage, q):
        pltpu.make_async_copy(src, dst, recv.at[min(Q * stage + q, LAST)]).start()

    def arrive(stage, q):
        ref = (
            buf_a.at[:, q], buf_b.at[:, q], got_b.at[:, q, :, :, :, real],
            got_c.at[:, q, :, :, :, real], mean.at[:, q, pl.ds(0, 3), :, :, real],
            got_e.at[:, q, :, :, :, real], buf_y.at[:, q], buf_z,
        )[stage]
        pltpu.make_async_copy(ref, ref, recv.at[min(Q * stage + q, LAST)]).wait()

    def axes(t):
        return t, (t + 1) % 3, (t + 2) % 3

    order = ((2, 0), (2, 1), (1, 0), (3, 0), (1, 1), (3, 1), (0, 1))
    row = lax.broadcasted_iota(jnp.int32, (4, PART, 128), 1)
    pairs = [(t, h) for t in range(3) for h in range(2)]

    def send_a(q):
        for t in range(3):
            mine = me[t] * 2 + me[3]
            local(x_ref.at[pl.ds(t * tiles + q * chunk + mine * na, na)], buf_a.at[t, q, mine], 0, q)
        for step, core in order:
            for t in range(3):
                to = peer(me, t, step, core)
                mine, theirs = me[t] * 2 + me[3], to[t] * 2 + to[3]
                remote(x_ref.at[pl.ds(t * tiles + q * chunk + theirs * na, na)], buf_a.at[t, q, mine], 0, q, to)

    def send_b1(q):
        arrive(0, q)
        for t, h in pairs:
            one, _, u, _ = halving(me, axes(t)[1], h)
            remote(buf_a.at[t, q, :, pl.ds(h * nh + (1 - u) * nu, nu)], buf_b.at[t, q, h], 1, q, one)

    def send_b2(q):
        arrive(1, q)
        for t in range(3):
            sums = []
            for h in range(2):
                _, _, u, v = halving(me, axes(t)[1], h)
                columns = []
                for half in (1 - v, v):
                    for n in range(nv):
                        k = half * nv + n
                        mine = buf_a[t, q, :, h * nh + u * nu + k].reshape(64, 128)
                        theirs = buf_b[t, q, h, :, k].reshape(64, 128)
                        columns.append(jnp.concatenate([mine, theirs], axis=0))
                sums.append(dot3(base_t[t, h], jnp.concatenate(columns, axis=1) - MIDDLE))
            for h in range(2):
                for n in range(nv):
                    for j in range(4):
                        rows = slice(PART * j, PART * (j + 1))
                        part[t, q, h, j, n] = sums[h][rows, 128 * n : 128 * (n + 1)]
                        kept[t, q, j, h, n] = sums[h][rows, 128 * (nv + n) : 128 * (nv + n + 1)]
        for t, h in pairs:
            two = halving(me, axes(t)[1], h)[1]
            remote(part.at[t, q, h, :, :, real], got_b.at[t, q, h, :, :, real], 2, q, two)

    def send_c(q):
        arrive(2, q)
        for t in range(3):
            for h in range(2):
                for j in range(4):
                    kept[t, q, j, h] += got_b[t, q, h, j]
        for t in range(3):
            c = axes(t)[2]
            for step in (2, 1, 3):
                to = peer(me, c, step)
                remote(kept.at[t, q, to[c], :, :, real], got_c.at[t, q, step - 1, :, :, real], 3, q, to)

    def send_d(q):
        arrive(3, q)
        for t in range(3):
            c = axes(t)[2]
            total = (kept[t, q, me[c]] + got_c[t, q, 0]) + (got_c[t, q, 1] + got_c[t, q, 2])
            mean[t, q, me[c]] = total / counts[me[c]][None, None]
        for t in range(3):
            c = axes(t)[2]
            for step in (2, 1, 3):
                to = peer(me, c, step)
                remote(mean.at[t, q, me[c], :, :, real], mean.at[t, q, me[c], :, :, real], 4, q, to)

    def send_e2(q):
        arrive(4, q)
        for t in range(3):
            for h in range(2):
                two = halving(me, axes(t)[1], h)[1]
                remote(mean.at[t, q, :, h, :, real], got_e.at[t, q, h, :, :, real], 5, q, two)

    def send_e1(q):
        arrive(5, q)
        for t in range(3):
            chosen = []
            for h in range(2):
                rows = jnp.concatenate(
                    [jnp.where(row < REAL, mean[t, q, :, h, n], 0.0).reshape(ROWS, 128) for n in range(nv)]
                    + [jnp.where(row < REAL, got_e[t, q, h, :, n], 0.0).reshape(ROWS, 128) for n in range(nv)],
                    axis=1,
                )
                rows = jnp.concatenate([rows, jnp.zeros((128 - ROWS, 128 * nu), F32)], axis=0)
                chosen.append(dot3(member[t, h], rows))
            for h in range(2):
                v = halving(me, axes(t)[1], h)[3]
                for k in range(nu):
                    to = (v if k < nv else 1 - v) * nv + k % nv
                    column = chosen[h][64:, 128 * k : 128 * (k + 1)]
                    buf_y[t, q, h, :, to] = (buf_b[t, q, h, :, to] - MIDDLE) - column.reshape(8, 8, 128)
            for h in range(2):
                _, _, u, v = halving(me, axes(t)[1], h)
                at = h * nh + u * nu
                for k in range(nu):
                    to = at + (v if k < nv else 1 - v) * nv + k % nv
                    column = chosen[h][:64, 128 * k : 128 * (k + 1)]
                    buf_z[t, q, :, to] = (buf_a[t, q, :, to] - MIDDLE) - column.reshape(8, 8, 128)
        for t, h in pairs:
            one, _, u, _ = halving(me, axes(t)[1], h)
            remote(buf_y.at[t, q, h], buf_z.at[t, q, :, pl.ds(h * nh + u * nu, nu)], 6, q, one)

    def send_f(q):
        arrive(6, q)
        for t in range(3):
            mine = me[t] * 2 + me[3]
            here = out_ref.at[pl.ds(t * tiles + q * chunk + mine * na, na)]
            for step, core in order:
                to = peer(me, t, step, core)
                remote(buf_z.at[t, q, to[t] * 2 + to[3]], here, 7, q, to)
            local(buf_z.at[t, q, mine], here, 7, q)

    def place(group):
        return group + jnp.where(group < REAL, 0, 1)

    def prepare():
        for load in loads:
            load.wait()
        group = lax.broadcasted_iota(jnp.int32, (HALF, 128), 0)
        seen = jnp.zeros((HALF, 128), F32)
        for r in range(4):
            days_row = jnp.where(year_row[r : r + 1] < BASE_YEARS, place(bucket_row[r : r + 1]), -1)
            seen = seen + jnp.where(days_row == group, 1.0, 0.0)
        number = jnp.maximum(jnp.sum(seen, axis=1, keepdims=True), 1.0)
        number = jnp.broadcast_to(number, (HALF, 128))
        for j in range(4):
            at = (j % 2) * PART
            counts[j] = number[at : at + PART]
        sub = lax.broadcasted_iota(jnp.int32, (8, 128), 0)
        lane = lax.broadcasted_iota(jnp.int32, (8, 128), 1)
        day, column = lax.rem(sub, 4), lane - lax.div(sub, 4) * HALF

        def pick(v):
            chosen = jnp.where(day == 0, v[0], jnp.where(day == 1, v[1], jnp.where(day == 2, v[2], v[3])))
            return jnp.where(chosen == column, 1.0, 0.0)

        def line(at, a):
            every, based = [], []
            for i in range(8):
                who = list(at)
                who[a], who[3] = i // 2, i % 2
                tm, space = device(*who)
                first = (tm * 16 + space) * 4
                groups = [place(bucket[first + d]) for d in range(4)]
                every.append(pick(groups))
                based.append(pick([jnp.where(year[first + d] < BASE_YEARS, groups[d], -1000) for d in range(4)]))
            return every, based

        for t in range(3):
            a, b, _ = axes(t)
            mine, mine_base = line(me, a)
            for h in range(2):
                theirs, theirs_base = line(halving(me, b, h)[0], a)
                every = jnp.concatenate(mine + theirs, axis=0).astype(BF16)
                based = jnp.concatenate(mine_base + theirs_base, axis=0).T[:ROWS].astype(BF16)
                member[t, h] = jnp.concatenate([every] * 3, axis=1)
                base_t[t, h] = jnp.concatenate([based] * 3, axis=1)

    stages = (send_a, send_b1, send_b2, send_c, send_d, send_e2, send_e1, send_f)
    stages[0](0)
    stages[0](1)
    stages[0](2)
    prepare()
    stages[1](0)
    stages[0](3)
    stages[1](1)
    stages[1](2)
    stages[1](3)
    stages[2](0)
    stages[2](1)
    stages[2](2)
    stages[2](3)
    stages[3](0)
    stages[3](1)
    stages[3](2)
    stages[3](3)
    stages[4](0)
    stages[4](1)
    stages[4](2)
    stages[4](3)
    stages[5](0)
    stages[5](1)
    stages[5](2)
    stages[5](3)
    stages[6](0)
    stages[6](1)
    stages[6](2)
    stages[6](3)
    stages[7](0)
    stages[7](1)
    stages[7](2)
    stages[7](3)
    arrive(7, 0)

    for stage, ref in (
        (0, buf_a.at[:, :, pl.ds(0, 7)]), (1, buf_b), (2, got_b.at[:, :, :, :, :, real]), (3, got_c.at[:, :, :, :, :, real]),
        (4, got_c.at[:, :, :, :, :, real]), (5, got_e.at[:, :, :, :, :, real]), (6, buf_b), (7, buf_z.at[:, :, pl.ds(0, 7)]),
    ):
        pltpu.make_async_copy(ref, ref, sent.at[0]).wait()


def shards(thermal_field, seasonal_bucket, season_of_record):
    days_here, cells = thermal_field.shape
    blocks = cells // 128
    x = thermal_field.reshape(days_here, blocks, 128).transpose(1, 0, 2)
    x = x.reshape(blocks // 2, 2 * days_here, 128)
    tiles = blocks // 2 // 3
    na, nv = tiles // Q // 8, tiles // Q // 64
    hbm = pl.BlockSpec(memory_space=pl.ANY)
    out = pl.pallas_call(
        kernel,
        out_shape=pltpu.VMEM(x.shape, F32),
        in_specs=[hbm] * 5,
        out_specs=hbm,
        scratch_shapes=[
            pltpu.VMEM((3, Q, 8, na, 8, 128), F32),
            pltpu.VMEM((3, Q, 2, 8, na // 4, 8, 128), F32),
            pltpu.VMEM((3, Q, 2, 4, nv, PART, 128), F32),
            pltpu.VMEM((3, Q, 4, 2, nv, PART, 128), F32),
            pltpu.VMEM((3, Q, 2, 4, nv, PART, 128), F32),
            pltpu.VMEM((3, Q, 3, 2, nv, PART, 128), F32),
            pltpu.VMEM((3, Q, 4, 2, nv, PART, 128), F32),
            pltpu.VMEM((3, Q, 2, 4, nv, PART, 128), F32),
            pltpu.VMEM((3, Q, 2, 8, na // 4, 8, 128), F32),
            pltpu.VMEM((3, Q, 8, na, 8, 128), F32),
            pltpu.VMEM((3, 2, 128, 384), BF16),
            pltpu.VMEM((3, 2, ROWS, 384), BF16),
            pltpu.VMEM((4, PART, 128), F32),
            pltpu.VMEM((4, 128), jnp.int32),
            pltpu.VMEM((4, 128), jnp.int32),
            pltpu.SMEM((512,), jnp.int32),
            pltpu.SMEM((512,), jnp.int32),
            pltpu.SemaphoreType.DMA((LAST + 1,)),
            pltpu.SemaphoreType.DMA((1,)),
            pltpu.SemaphoreType.DMA((4,)),
        ],
        compiler_params=pltpu.CompilerParams(
            collective_id=0, has_side_effects=True, vmem_limit_bytes=63_880_000
        ),
    )(
        x,
        seasonal_bucket.reshape(4, 128),
        season_of_record.reshape(4, 128),
        seasonal_bucket,
        season_of_record,
    )
    out = out.reshape(blocks, days_here, 128).transpose(1, 0, 2)
    return out.reshape(days_here, cells)


def solution(mesh):
    placed = (P(("tm", "space"), None), P(), P())
    return jax.shard_map(
        shards, mesh=mesh, in_specs=placed, out_specs=P(("tm", "space"), None), check_vma=False
    )
```

```python
import functools

import jax
import jax.numpy as jnp
from jax import lax
from jax.experimental import pallas as pl
from jax.experimental.pallas import tpu as pltpu
from jax.sharding import PartitionSpec as P

GROUPS = 46
BASE_YEARS = 6
MIDDLE = 250.0
MESH = pl.DeviceIdType.MESH
F32, BF16 = jnp.float32, jnp.bfloat16

Q = 4
LAST = 7 * Q
HALF = 48
ROWS = 2 * HALF
PART = ROWS // 4
REAL = GROUPS // 2


def coordinates():
    tm, space = lax.axis_index("tm"), lax.axis_index("space")
    x = lax.rem(lax.div(space, 2), 2) * 2 + lax.div(tm, 4)
    return (x, lax.rem(tm, 4), lax.div(space, 4), lax.rem(space, 2))


def device(x, y, z, core):
    return (lax.rem(x, 2) * 4 + y, z * 4 + lax.div(x, 2) * 2 + core)


def peer(me, axis, step, core_step=0):
    at = list(me)
    at[axis] = lax.rem(me[axis] + step, 4)
    at[3] = lax.rem(me[3] + core_step, 2)
    return at


def dot3(one_hot_thrice, v):
    high = v.astype(BF16)
    rest = v - high.astype(F32)
    middle = rest.astype(BF16)
    low = (rest - middle.astype(F32)).astype(BF16)
    return jnp.dot(one_hot_thrice, jnp.concatenate([high, middle, low], axis=0), preferred_element_type=F32)


def halving(at, axis, h):
    m = at[axis]
    up = lax.rem(m + h, 2) == 0
    one, two = jnp.where(up, 1, 3), jnp.where(up, 3, 1)
    u = lax.rem(lax.div(m + 1 - h, 2), 2)
    v = lax.rem(m, 2) if h else lax.div(m, 2)
    return peer(at, axis, one), peer(at, axis, two), u, v


def kernel(
    x_ref, bucket_rows, year_rows, bucket_hbm, year_hbm, out_ref,
    buf_a, buf_b, part, kept, got_b, got_c, mean, got_e, buf_y, buf_z,
    member, base_t, counts, bucket_row, year_row, bucket, year, recv, sent, small,
):
    me = coordinates()
    tiles = x_ref.shape[0] // 3
    chunk = tiles // Q
    na = chunk // 8
    nh, nu, nv = na // 2, na // 4, na // 8
    real = pl.ds(0, REAL)

    loads = [
        pltpu.make_async_copy(src, dst, small.at[i])
        for i, (src, dst) in enumerate(
            ((bucket_hbm, bucket), (year_hbm, year), (bucket_rows, bucket_row), (year_rows, year_row))
        )
    ]
    for load in loads:
        load.start()

    barrier = pltpu.get_barrier_semaphore()
    partners = 0
    for axis in range(3):
        for step in (2, 1, 3):
            for core in range(2):
                pl.semaphore_signal(barrier, inc=1, device_id=device(*peer(me, axis, step, core)), device_id_type=MESH)
                partners += 1
    pl.semaphore_signal(barrier, inc=1, device_id=device(*peer(me, 0, 0, 1)), device_id_type=MESH)
    pl.semaphore_wait(barrier, partners + 1)

    def remote(src, dst, stage, q, to):
        pltpu.make_async_remote_copy(
            src_ref=src, dst_ref=dst, send_sem=sent.at[0], recv_sem=recv.at[min(Q * stage + q, LAST)],
            device_id=device(*to), device_id_type=MESH,
        ).start()

    def local(src, dst, stage, q):
        pltpu.make_async_copy(src, dst, recv.at[min(Q * stage + q, LAST)]).start()

    def arrive(stage, q):
        ref = (
            buf_a.at[:, q], buf_b.at[:, q], got_b.at[:, q, :, :, :, real],
            got_c.at[:, q, :, :, :, real], mean.at[:, q, pl.ds(0, 3), :, :, real],
            got_e.at[:, q, :, :, :, real], buf_y.at[:, q], buf_z,
        )[stage]
        pltpu.make_async_copy(ref, ref, recv.at[min(Q * stage + q, LAST)]).wait()

    def axes(t):
        return t, (t + 1) % 3, (t + 2) % 3

    order = ((2, 0), (2, 1), (1, 0), (3, 0), (1, 1), (3, 1), (0, 1))
    row = lax.broadcasted_iota(jnp.int32, (4, PART, 128), 1)
    pairs = [(t, h) for t in range(3) for h in range(2)]

    def send_a(q):
        for step, core in order:
            for t in range(3):
                to = peer(me, t, step, core)
                mine, theirs = me[t] * 2 + me[3], to[t] * 2 + to[3]
                remote(x_ref.at[pl.ds(t * tiles + q * chunk + theirs * na, na)], buf_a.at[t, q, mine], 0, q, to)
        for t in range(3):
            mine = me[t] * 2 + me[3]
            local(x_ref.at[pl.ds(t * tiles + q * chunk + mine * na, na)], buf_a.at[t, q, mine], 0, q)

    def send_b1(q):
        arrive(0, q)
        for t, h in pairs:
            one, _, u, _ = halving(me, axes(t)[1], h)
            remote(buf_a.at[t, q, :, pl.ds(h * nh + (1 - u) * nu, nu)], buf_b.at[t, q, h], 1, q, one)

    def send_b2(q):
        arrive(1, q)
        for t in range(3):
            sums = []
            for h in range(2):
                _, _, u, v = halving(me, axes(t)[1], h)
                columns = []
                for half in (1 - v, v):
                    for n in range(nv):
                        k = half * nv + n
                        mine = buf_a[t, q, :, h * nh + u * nu + k].reshape(64, 128)
                        theirs = buf_b[t, q, h, :, k].reshape(64, 128)
                        columns.append(jnp.concatenate([mine, theirs], axis=0))
                sums.append(dot3(base_t[t, h], jnp.concatenate(columns, axis=1) - MIDDLE))
            for h in range(2):
                for n in range(nv):
                    for j in range(4):
                        rows = slice(PART * j, PART * (j + 1))
                        part[t, q, h, j, n] = sums[h][rows, 128 * n : 128 * (n + 1)]
                        kept[t, q, j, h, n] = sums[h][rows, 128 * (nv + n) : 128 * (nv + n + 1)]
        for t, h in pairs:
            two = halving(me, axes(t)[1], h)[1]
            remote(part.at[t, q, h, :, :, real], got_b.at[t, q, h, :, :, real], 2, q, two)

    def send_c(q):
        arrive(2, q)
        for t in range(3):
            for h in range(2):
                for j in range(4):
                    kept[t, q, j, h] += got_b[t, q, h, j]
        for t in range(3):
            c = axes(t)[2]
            for step in (2, 1, 3):
                to = peer(me, c, step)
                remote(kept.at[t, q, to[c], :, :, real], got_c.at[t, q, step - 1, :, :, real], 3, q, to)

    def send_d(q):
        arrive(3, q)
        for t in range(3):
            c = axes(t)[2]
            total = (kept[t, q, me[c]] + got_c[t, q, 0]) + (got_c[t, q, 1] + got_c[t, q, 2])
            mean[t, q, me[c]] = total / counts[me[c]][None, None]
        for t in range(3):
            c = axes(t)[2]
            for step in (2, 1, 3):
                to = peer(me, c, step)
                remote(mean.at[t, q, me[c], :, :, real], mean.at[t, q, me[c], :, :, real], 4, q, to)

    def send_e2(q):
        arrive(4, q)
        for t in range(3):
            for h in range(2):
                two = halving(me, axes(t)[1], h)[1]
                remote(mean.at[t, q, :, h, :, real], got_e.at[t, q, h, :, :, real], 5, q, two)

    def send_e1(q):
        arrive(5, q)
        for t in range(3):
            chosen = []
            for h in range(2):
                rows = jnp.concatenate(
                    [jnp.where(row < REAL, mean[t, q, :, h, n], 0.0).reshape(ROWS, 128) for n in range(nv)]
                    + [jnp.where(row < REAL, got_e[t, q, h, :, n], 0.0).reshape(ROWS, 128) for n in range(nv)],
                    axis=1,
                )
                rows = jnp.concatenate([rows, jnp.zeros((128 - ROWS, 128 * nu), F32)], axis=0)
                chosen.append(dot3(member[t, h], rows))
            for h in range(2):
                v = halving(me, axes(t)[1], h)[3]
                for k in range(nu):
                    to = (v if k < nv else 1 - v) * nv + k % nv
                    column = chosen[h][64:, 128 * k : 128 * (k + 1)]
                    buf_y[t, q, h, :, to] = (buf_b[t, q, h, :, to] - MIDDLE) - column.reshape(8, 8, 128)
            for h in range(2):
                _, _, u, v = halving(me, axes(t)[1], h)
                at = h * nh + u * nu
                for k in range(nu):
                    to = at + (v if k < nv else 1 - v) * nv + k % nv
                    column = chosen[h][:64, 128 * k : 128 * (k + 1)]
                    buf_z[t, q, :, to] = (buf_a[t, q, :, to] - MIDDLE) - column.reshape(8, 8, 128)
        for t, h in pairs:
            one, _, u, _ = halving(me, axes(t)[1], h)
            remote(buf_y.at[t, q, h], buf_z.at[t, q, :, pl.ds(h * nh + u * nu, nu)], 6, q, one)

    def send_f(q):
        arrive(6, q)
        for t in range(3):
            mine = me[t] * 2 + me[3]
            here = out_ref.at[pl.ds(t * tiles + q * chunk + mine * na, na)]
            for step, core in order:
                to = peer(me, t, step, core)
                remote(buf_z.at[t, q, to[t] * 2 + to[3]], here, 7, q, to)
            local(buf_z.at[t, q, mine], here, 7, q)

    def place(group):
        return group + jnp.where(group < REAL, 0, 1)

    def prepare():
        for load in loads:
            load.wait()
        group = lax.broadcasted_iota(jnp.int32, (HALF, 128), 0)
        seen = jnp.zeros((HALF, 128), F32)
        for r in range(4):
            days_row = jnp.where(year_row[r : r + 1] < BASE_YEARS, place(bucket_row[r : r + 1]), -1)
            seen = seen + jnp.where(days_row == group, 1.0, 0.0)
        number = jnp.maximum(jnp.sum(seen, axis=1, keepdims=True), 1.0)
        number = jnp.broadcast_to(number, (HALF, 128))
        for j in range(4):
            at = (j % 2) * PART
            counts[j] = number[at : at + PART]
        sub = lax.broadcasted_iota(jnp.int32, (8, 128), 0)
        lane = lax.broadcasted_iota(jnp.int32, (8, 128), 1)
        day, column = lax.rem(sub, 4), lane - lax.div(sub, 4) * HALF

        def pick(v):
            chosen = jnp.where(day == 0, v[0], jnp.where(day == 1, v[1], jnp.where(day == 2, v[2], v[3])))
            return jnp.where(chosen == column, 1.0, 0.0)

        def line(at, a):
            every, based = [], []
            for i in range(8):
                who = list(at)
                who[a], who[3] = i // 2, i % 2
                tm, space = device(*who)
                first = (tm * 16 + space) * 4
                groups = [place(bucket[first + d]) for d in range(4)]
                every.append(pick(groups))
                based.append(pick([jnp.where(year[first + d] < BASE_YEARS, groups[d], -1000) for d in range(4)]))
            return every, based

        for t in range(3):
            a, b, _ = axes(t)
            mine, mine_base = line(me, a)
            for h in range(2):
                theirs, theirs_base = line(halving(me, b, h)[0], a)
                every = jnp.concatenate(mine + theirs, axis=0).astype(BF16)
                based = jnp.concatenate(mine_base + theirs_base, axis=0).T[:ROWS].astype(BF16)
                member[t, h] = jnp.concatenate([every] * 3, axis=1)
                base_t[t, h] = jnp.concatenate([based] * 3, axis=1)

    stages = (send_a, send_b1, send_b2, send_c, send_d, send_e2, send_e1, send_f)
    stages[0](0)
    stages[0](1)
    stages[0](2)
    prepare()
    stages[1](0)
    stages[0](3)
    stages[1](1)
    stages[1](2)
    stages[1](3)
    stages[2](0)
    stages[2](1)
    stages[2](2)
    stages[2](3)
    stages[3](0)
    stages[3](1)
    stages[3](2)
    stages[3](3)
    stages[4](0)
    stages[4](1)
    stages[4](2)
    stages[4](3)
    stages[5](0)
    stages[5](1)
    stages[5](2)
    stages[5](3)
    stages[6](0)
    stages[6](1)
    stages[6](2)
    stages[6](3)
    stages[7](0)
    stages[7](1)
    stages[7](2)
    stages[7](3)
    arrive(7, 0)

    for stage, ref in (
        (0, buf_a.at[:, :, pl.ds(0, 7)]), (1, buf_b), (2, got_b.at[:, :, :, :, :, real]), (3, got_c.at[:, :, :, :, :, real]),
        (4, got_c.at[:, :, :, :, :, real]), (5, got_e.at[:, :, :, :, :, real]), (6, buf_b), (7, buf_z.at[:, :, pl.ds(0, 7)]),
    ):
        pltpu.make_async_copy(ref, ref, sent.at[0]).wait()


def shards(thermal_field, seasonal_bucket, season_of_record):
    days_here, cells = thermal_field.shape
    blocks = cells // 128
    x = thermal_field.reshape(days_here, blocks, 128).transpose(1, 0, 2)
    x = x.reshape(blocks // 2, 2 * days_here, 128)
    tiles = blocks // 2 // 3
    na, nv = tiles // Q // 8, tiles // Q // 64
    hbm = pl.BlockSpec(memory_space=pl.ANY)
    out = pl.pallas_call(
        kernel,
        out_shape=pltpu.VMEM(x.shape, F32),
        in_specs=[hbm] * 5,
        out_specs=hbm,
        scratch_shapes=[
            pltpu.VMEM((3, Q, 8, na, 8, 128), F32),
            pltpu.VMEM((3, Q, 2, 8, na // 4, 8, 128), F32),
            pltpu.VMEM((3, Q, 2, 4, nv, PART, 128), F32),
            pltpu.VMEM((3, Q, 4, 2, nv, PART, 128), F32),
            pltpu.VMEM((3, Q, 2, 4, nv, PART, 128), F32),
            pltpu.VMEM((3, Q, 3, 2, nv, PART, 128), F32),
            pltpu.VMEM((3, Q, 4, 2, nv, PART, 128), F32),
            pltpu.VMEM((3, Q, 2, 4, nv, PART, 128), F32),
            pltpu.VMEM((3, Q, 2, 8, na // 4, 8, 128), F32),
            pltpu.VMEM((3, Q, 8, na, 8, 128), F32),
            pltpu.VMEM((3, 2, 128, 384), BF16),
            pltpu.VMEM((3, 2, ROWS, 384), BF16),
            pltpu.VMEM((4, PART, 128), F32),
            pltpu.VMEM((4, 128), jnp.int32),
            pltpu.VMEM((4, 128), jnp.int32),
            pltpu.SMEM((512,), jnp.int32),
            pltpu.SMEM((512,), jnp.int32),
            pltpu.SemaphoreType.DMA((LAST + 1,)),
            pltpu.SemaphoreType.DMA((1,)),
            pltpu.SemaphoreType.DMA((4,)),
        ],
        compiler_params=pltpu.CompilerParams(
            collective_id=0, has_side_effects=True, vmem_limit_bytes=63_880_000
        ),
    )(
        x,
        seasonal_bucket.reshape(4, 128),
        season_of_record.reshape(4, 128),
        seasonal_bucket,
        season_of_record,
    )
    out = out.reshape(blocks, days_here, 128).transpose(1, 0, 2)
    return out.reshape(days_here, cells)


def solution(mesh):
    placed = (P(("tm", "space"), None), P(), P())
    return jax.shard_map(
        shards, mesh=mesh, in_specs=placed, out_specs=P(("tm", "space"), None), check_vma=False
    )
```
